32 devices in a mesh: pair: 4 (over y, x), grow: 4 (over z), gcol: 2 (over core).
Axes of the slice: x: 2, y: 2, z: 4, core: 2. Of those that a mesh axis runs over, the one named last changes fastest.
Arguments:
- valence: bfloat16 [16, 96, 9216], P(None, 'grow'), may hold values from -6 to 6
- conduction: bfloat16 [16, 96, 9216], P(('pair', 'gcol'), 'grow'), may hold values from -6 to 6
- val_energy: float32 [16], replicated, may hold values from -10 to -1
- cond_energy: float32 [16], replicated, may hold values from 1 to 20
- val_occupation: int32 [16], replicated, may hold values from 1 to 16
- gvectors: int32 [3, 3840], replicated, may hold values from -12 to 12, as said below
Outputs:
- chi_zero: float32 [7680, 7680], P(('pair', 'gcol'), 'grow')
The draws below stay inside these ranges and needn't reach their ends.
Inputs may be any that keep to these rules, and one draw needn't show every extreme that they name: gvectors holds 3840 distinct wave vectors; the first component lies in 1 .. 12, the other two in -12 .. 12.
All inputs are finite; a program needn't handle non-finite values.
Results may differ from the reference program's by a relative error of at most 0.02.
Values may be sent and summed in bfloat16 or wider, within the bound.
A program may use at most 128 MiB of HBM per device.

```python
import math
import jax
import jax.numpy as jnp
from jax import lax

N = 96
RAD = 12
KG = 3840
NV = 16
NCOND = 16
NPAIRS = 256
N_GROW = 4


def draw_gvectors(key, part):
    extent = 2 * RAD + 1
    total_count = RAD * extent * extent
    chosen = jax.random.permutation(jax.random.fold_in(key, 11), total_count)[:KG]
    component_a = chosen // (extent * extent) + 1
    component_b = chosen // extent % extent - RAD
    component_c = chosen % extent - RAD
    return jnp.stack([component_a, component_b, component_c]).astype(jnp.int32)


def touch_ends(array, key, low, top_value):
    place = [jax.random.randint(jax.random.fold_in(key, axis), (), 0, length) for axis, length in enumerate(array.shape)]
    main_axis = array.shape.index(max(array.shape))
    neighbour = place[:main_axis] + [(place[main_axis] + 1) % array.shape[main_axis]] + place[main_axis + 1:]
    return array.at[tuple(place)].set(low).at[tuple(neighbour)].set(top_value)


def steps_of(rng, shape, pieces, low, top_value):
    def one(axis_at, parts):
        steps = jax.random.uniform(jax.random.fold_in(jax.random.fold_in(rng, 6), axis_at), (parts,), jnp.float32, low / len(pieces), top_value / len(pieces))
        return jnp.repeat(jnp.exp(steps), shape[axis_at] // parts).reshape((-1,) + (1,) * (len(shape) - axis_at - 1))

    level = one(*pieces[0])
    for cut in pieces[1:]:
        level = level * one(*cut)
    return level


def scatter_about(key, shape, deviation, reach, cuts=(), kind=jnp.bfloat16):
    gain = steps_of(key, shape, cuts, -0.22, 0.18) if cuts else 1.0
    array = jax.random.normal(key, shape, jnp.float32) * deviation * gain
    return jnp.minimum(jnp.maximum(array, -reach), reach).astype(kind)


def setup_inputs(seed: int = 0) -> dict:
    arg_keys = jax.random.split(jax.random.key(seed), 7)
    valence = scatter_about(arg_keys[0], (NV, N, N * N), 1.0, 6.0, ((1, 4),))
    conduction = scatter_about(arg_keys[1], (NCOND, N, N * N), 1.0, 6.0, ((0, 8), (1, 4)))
    val_energy = jnp.clip(jax.random.uniform(arg_keys[2], (NV,), jnp.float32, -10.0, -1.0), -10.0, -1.0)
    cond_energy = jnp.clip(jax.random.uniform(arg_keys[3], (NCOND,), jnp.float32, 1.0, 20.0), 1.0, 20.0)
    val_occupation = touch_ends(jax.random.randint(arg_keys[4], (NV,), 1, 17), jax.random.fold_in(arg_keys[4], 1), 1, 16).astype(jnp.int32)
    gvectors = draw_gvectors(jax.random.fold_in(arg_keys[6], 71), 0)
    return dict(valence=valence, conduction=conduction, val_energy=val_energy, cond_energy=cond_energy, val_occupation=val_occupation, gvectors=gvectors)


def wave_tables(positions, frequencies):
    phases = jnp.mod(positions[:, None] * frequencies[None, :], N).astype(jnp.float32) * (2.0 * math.pi / N)
    return (jnp.cos(phases), jnp.sin(phases))

def build_tables(x_positions):
    all_freq = jnp.arange(-RAD, RAD + 1, dtype=jnp.int32)
    pos_freq = jnp.arange(1, RAD + 1, dtype=jnp.int32)
    positions = jnp.arange(N, dtype=jnp.int32)
    cosine, sine_part = wave_tables(positions, all_freq)
    z_table = jnp.concatenate([cosine, sine_part], 1).astype(jnp.bfloat16)
    y_table = jnp.stack([jnp.stack([cosine, sine_part], 1), jnp.stack([-sine_part, cosine], 1)], 1).astype(jnp.bfloat16)
    x_cos, x_sin = wave_tables(x_positions, pos_freq)
    x_table = jnp.stack([jnp.stack([x_cos, -x_sin], 1), jnp.stack([-x_sin, -x_cos], 1)], 1).astype(jnp.bfloat16)
    return (z_table, y_table, x_table)

def band_transform(one_band, valence, z_table, y_table, x_table, flat_index):
    extent = 2 * RAD + 1
    planes = N // N_GROW
    density = valence * one_band[None]
    section_one = jnp.dot(density.reshape(-1, N), z_table, preferred_element_type=jnp.float32).astype(jnp.bfloat16)
    section_one = section_one.reshape(NV * N, N, 2, extent)
    second = jnp.einsum('ayik,yioj->aojk', section_one.astype(jnp.float32), y_table.astype(jnp.float32)).astype(jnp.bfloat16)
    second = second.reshape(NV, N_GROW, planes, 2, extent * extent)
    block_table = x_table.reshape(N_GROW, planes, 2, 2, RAD)
    blocks = jnp.einsum('pbxoq,bxosm->pbsmq', second.astype(jnp.float32), block_table.astype(jnp.float32))
    rounded = lax.optimization_barrier(blocks.astype(jnp.bfloat16))
    section_three = lax.optimization_barrier(jnp.sum(rounded.astype(jnp.float32), axis=1))
    section_three = section_three.reshape(NV, 2, RAD * extent * extent)
    picked = jnp.take(section_three, flat_index, axis=2)
    return picked.reshape(NV, 2 * KG)

def reference(valence, conduction, val_energy, cond_energy, val_occupation, gvectors):
    extent = 2 * RAD + 1
    z_table, y_table, x_table = build_tables(jnp.arange(N, dtype=jnp.int32))
    flat_index = (((gvectors[0] - 1) * extent + gvectors[1] + RAD) * extent + gvectors[2] + RAD).astype(jnp.int32)
    weight = val_occupation.astype(jnp.float32)[None, :] / (4.0 * (cond_energy[:, None] - val_energy[None, :]))
    factor = jnp.sqrt(weight) * (1.0 / N ** 1.5)

    def per_band(inputs):
        one_band, band_factor = inputs
        picked = band_transform(one_band, valence, z_table, y_table, x_table, flat_index)
        return (picked * band_factor[:, None]).astype(jnp.bfloat16)
    weighted = lax.map(per_band, (conduction, factor))
    flattened = weighted.reshape(-1, 2 * KG)
    chi_block = lax.dot_general(flattened, flattened, (((0,), (0,)), ((), ())), preferred_element_type=jnp.float32)
    return chi_block * (-1.0 / math.sqrt(NPAIRS))
```

```python
import functools
import math

import jax
import jax.numpy as jnp
import numpy as np
from jax import lax
from jax.experimental import pallas as pl
from jax.experimental.pallas import tpu as pltpu
from jax.sharding import PartitionSpec as P

N = 96
RAD = 12
KG = 3840
NV = 16


def wave_tables(positions, frequencies):
    phases = jnp.mod(positions[:, None] * frequencies[None, :], N).astype(jnp.float32) * (
        2.0 * math.pi / N
    )
    return (jnp.cos(phases), jnp.sin(phases))


def build_tables(x_positions):
    all_freq = jnp.arange(-RAD, RAD + 1, dtype=jnp.int32)
    pos_freq = jnp.arange(1, RAD + 1, dtype=jnp.int32)
    positions = jnp.arange(N, dtype=jnp.int32)
    cosine, sine_part = wave_tables(positions, all_freq)
    z_table = jnp.concatenate([cosine, sine_part], 1).astype(jnp.bfloat16)
    y_table = jnp.stack(
        [jnp.stack([cosine, sine_part], 1), jnp.stack([-sine_part, cosine], 1)], 1
    ).astype(jnp.bfloat16)
    x_cos, x_sin = wave_tables(x_positions, pos_freq)
    x_table = jnp.stack([jnp.stack([x_cos, -x_sin], 1), jnp.stack([-x_sin, -x_cos], 1)], 1).astype(
        jnp.bfloat16
    )
    return (z_table, y_table, x_table)


def pair_product(left_rows, right_rows):
    return lax.dot_general(
        left_rows, right_rows, (((0,), (0,)), ((), ())), preferred_element_type=jnp.float32
    )


def body(valence, conduction, val_energy, cond_energy, val_occupation, gvectors):
    pair_count = lax.axis_size("pair")
    gcol_count = lax.axis_size("gcol")
    planes = valence.shape[1]
    cond_bands = conduction.shape[0]
    extent = 2 * RAD + 1
    local_pairs = cond_bands * NV
    x_positions = lax.axis_index("grow") * planes + jnp.arange(planes, dtype=jnp.int32)
    z_table, y_table, x_table = build_tables(x_positions)
    flat_index = ((gvectors[0] - 1) * extent + gvectors[1] + RAD) * extent + gvectors[2] + RAD
    density = conduction[:, None] * valence[None]
    section_one = jnp.dot(
        density.reshape(-1, N), z_table, preferred_element_type=jnp.float32
    ).astype(jnp.bfloat16)
    section_one = section_one.reshape(local_pairs * planes, N, 2, extent)
    second = jnp.einsum(
        "ayik,yioj->aojk", section_one, y_table, preferred_element_type=jnp.float32
    ).astype(jnp.bfloat16)
    second = second.reshape(local_pairs, planes, 2, extent * extent)
    section_three = jnp.einsum(
        "pxoq,xosm->psmq", second, x_table, preferred_element_type=jnp.float32
    )
    section_three = section_three.reshape(local_pairs, 2, RAD * extent * extent)
    picked = jnp.take(section_three, flat_index, axis=2).reshape(local_pairs, 2 * KG)
    summed = lax.psum_scatter(
        picked.astype(jnp.bfloat16), "grow", scatter_dimension=1, tiled=True
    ).astype(jnp.float32)
    first_band = (lax.axis_index("pair") * gcol_count + lax.axis_index("gcol")) * cond_bands
    own_energy = lax.dynamic_slice_in_dim(cond_energy, first_band, cond_bands, 0)
    weight = val_occupation.astype(jnp.float32)[None, :] / (
        4.0 * (own_energy[:, None] - val_energy[None, :])
    )
    factor = (jnp.sqrt(weight) * (1.0 / N**1.5)).reshape(local_pairs, 1)
    weighted = (summed * factor).astype(jnp.bfloat16)
    prefactor = -1.0 / math.sqrt(pair_count * gcol_count * local_pairs)
    full_rows = lax.all_gather(weighted, "grow", axis=1, tiled=True)
    row_part = lax.all_to_all(full_rows, "pair", split_axis=1, concat_axis=0, tiled=True)
    partial_value = pair_product(row_part, lax.all_gather(weighted, "pair", axis=0, tiled=True))
    return lax.psum_scatter(
        (partial_value * prefactor).astype(jnp.bfloat16), "gcol", scatter_dimension=0, tiled=True
    ).astype(jnp.float32)


EXT = 2 * RAD + 1
QUARTER = N * N // 4
STEP = 8 * N
CLASSES = ((0, 4, 8, 12), (2, 6, 10), (1, 3, 5, 7, 9, 11))
WIDTHS = (128, 128, 256)
ROWS = (104, 80, 152)
STARTS = (0, 104, 184)
NR = 336
TALL = (112, 80, 160)
PIECE = 384
LAG = 3


def half_plane_tables():
    total = 2 * sum(WIDTHS)
    left = np.zeros((2, N // 4, total), np.float32)
    right = np.zeros((2, N, total), np.float32)
    sign = np.zeros((1, WIDTHS[2]), np.float32)
    y = np.arange(N // 4)[:, None]
    z = np.arange(N)[:, None]
    k = np.arange(-RAD, RAD + 1)
    base = 0
    for freqs, width in zip(CLASSES, WIDTHS):
        jj = np.repeat(np.array(freqs), EXT)[None]
        kk = np.tile(k, len(freqs))[None]
        count = jj.shape[1]
        ay = 2 * np.pi * ((jj * y) % N) / N
        az = 2 * np.pi * ((kk * z) % N) / N
        for part in range(2):
            cols = slice(base + part * width, base + part * width + count)
            left[0, :, cols] = np.sin(ay) if part else np.cos(ay)
            left[1, :, cols] = np.cos(ay) if part else -np.sin(ay)
            right[0, :, cols] = np.cos(az)
            right[1, :, cols] = np.sin(az)
        base += 2 * width
    jj = np.repeat(np.array(CLASSES[2]), EXT)
    sign[0, : jj.size] = np.where(jj % 4 == 1, 1.0, -1.0)
    return left, right, sign


def plane_table(pairs):
    x = np.arange(N)[:, None]
    a = np.arange(1, RAD + 1)[None]
    ang = 2 * np.pi * ((a * x) % N) / N
    c, s = np.cos(ang), np.sin(ang)
    tab = np.stack([np.stack([c, -s, c, -s], -1), np.stack([-s, -c, s, c], -1)])
    return np.repeat(tab.reshape(2, N, RAD * 4), pairs, axis=2).astype(np.float32)


def row_index(a, b, d):
    j = jnp.abs(b)
    k = jnp.where(b < 0, -d, d) + RAD
    row = jnp.where(
        (j & 1) == 1,
        STARTS[2] + (j >> 1) * EXT,
        jnp.where((j & 3) == 2, STARTS[1], STARTS[0]) + (j >> 2) * EXT,
    )
    return jnp.maximum((a - 1) * NR + row + k, 0)


def chi_kernel(
    occ, val_e, cond_e, gvec, val, cond, left, right, sign, xtab,
    cols_out, rows_out,
    vbuf, cbuf, leftv, rightv, signv, xv, tabs_e, tabs_o,
    ee0, eo0, od0, ee1, eo1, od1, acc_e, acc_o, xmat, sec, got,
    part, rin, lin, rout, lout, tot, cols, rows, index, idx,
    loads, chain_send, chain_recv, row_send, row_recv, col_send, col_recv,
    over_send, over_recv, outs,
):
    f32, bf16 = jnp.float32, jnp.bfloat16
    nv, planes, _ = val.shape
    bands = cond.shape[0]
    height = nv * planes
    pairs = bands * nv
    lanes = 128
    half = lanes // 2
    steps = QUARTER // STEP
    pieces = part.shape[0]
    slots, _, width = cols.shape
    count = slots // 2
    per = width // PIECE
    middle = per // 2
    span = rows.shape[2]
    low = width - span
    p, g, c = lax.axis_index("pair"), lax.axis_index("grow"), lax.axis_index("gcol")
    me = p * 2 + c
    turn = lambda at, k: lax.rem(at + k, count)

    def remote(src, dst, send, recv, to):
        return pltpu.make_async_remote_copy(
            src_ref=src, dst_ref=dst, send_sem=send, recv_sem=recv,
            device_id=to, device_id_type=pl.DeviceIdType.MESH,
        )

    table_loads = [
        pltpu.make_async_copy(a, b, loads.at[8 * steps + i])
        for i, (a, b) in enumerate(
            (
                (left, leftv),
                (right, rightv),
                (sign, signv),
                (xtab.at[:, pl.ds(pl.multiple_of(g * planes, 8), planes), :], xv),
            )
        )
    ]
    step_loads = []
    for s in range(steps):
        group = []
        for q in range(4):
            at = pl.ds(q * QUARTER + s * STEP, STEP)
            for u, (a, b) in enumerate(((cond, cbuf), (val, vbuf))):
                group.append(
                    pltpu.make_async_copy(
                        a.at[:, :, at], b.at[:, :, at], loads.at[8 * s + 2 * q + u]
                    )
                )
        step_loads.append(group)
    for copy in table_loads[:3]:
        copy.start()
    for copy in step_loads[0]:
        copy.start()
    table_loads[3].start()
    for group in step_loads[1:]:
        for copy in group:
            copy.start()

    barrier = pltpu.get_barrier_semaphore()
    pl.semaphore_signal(barrier, inc=1, device_id=(p, g, 1 - c))
    for k in range(1, count):
        for d in range(2):
            pl.semaphore_signal(barrier, inc=1, device_id=(turn(p, k), g, d))
        pl.semaphore_signal(barrier, inc=1, device_id=(p, turn(g, k), c))

    index[...] = row_index(gvec[0:1, :], gvec[1:2, :], gvec[2:3, :])
    index_copy = pltpu.make_async_copy(index, idx, outs.at[0])
    index_copy.start()

    for copy in table_loads[:3]:
        copy.wait()

    def table_rows(y, carry):
        l1 = leftv[0, pl.ds(y, 1), :]
        l2 = leftv[1, pl.ds(y, 1), :]
        full = l1 * rightv[0] + l2 * rightv[1]
        w = WIDTHS[2]
        odd_p, odd_q = full[:, 512 : 512 + w], full[:, 512 + w :]
        tabs_e[pl.ds(pl.multiple_of(y * N, 32), N), :] = full[:, 0:512].astype(bf16)
        s = y // (STEP // N)
        at = pl.multiple_of((y - s * (STEP // N)) * N, 32)
        tabs_o[s, pl.ds(at, N), 0:w] = odd_p.astype(bf16)
        tabs_o[s, pl.ds(at, N), w:] = odd_q.astype(bf16)
        tabs_o[s, pl.ds(STEP + at, N), 0:w] = (odd_q * (0.0 - signv[...])).astype(bf16)
        tabs_o[s, pl.ds(STEP + at, N), w:] = (odd_p * signv[...]).astype(bf16)
        return carry

    lax.fori_loop(0, QUARTER // N, table_rows, 0)

    def products(s, ee, eo, od):
        for copy in step_loads[s]:
            copy.wait()
        for b in range(bands):
            for m in range(STEP // lanes):
                at = [pl.ds(q * QUARTER + s * STEP + m * lanes, lanes) for q in range(4)]
                here = slice(m * lanes, (m + 1) * lanes)
                there = slice(STEP + m * lanes, STEP + (m + 1) * lanes)
                cs = [cbuf[b, :, q].astype(f32)[None] for q in at]
                for v in range(0, nv, 2):
                    d0, d1, d2, d3 = [
                        (vbuf[v : v + 2, :, q].astype(f32) * u).reshape(2 * planes, lanes)
                        for q, u in zip(at, cs)
                    ]
                    e0, e1 = d0 + d2, d1 + d3
                    row = b * height + v * planes
                    where = slice(row, row + 2 * planes)
                    ee[where, here] = (e0 + e1).astype(bf16)
                    eo[where, here] = (e0 - e1).astype(bf16)
                    od[where, here] = (d0 - d2).astype(bf16)
                    od[where, there] = (d1 - d3).astype(bf16)

    def multiply(s, ee, eo, od):
        at = slice(s * STEP, (s + 1) * STEP)
        parts = (
            (acc_e, slice(0, 256), jnp.dot(ee[...], tabs_e[at, 0:256], preferred_element_type=f32)),
            (acc_e, slice(256, 512), jnp.dot(eo[...], tabs_e[at, 256:512], preferred_element_type=f32)),
            (acc_o, slice(0, 512), jnp.dot(od[...], tabs_o[s], preferred_element_type=f32)),
        )
        for acc, where, value in parts:
            if s:
                acc[:, where] += value
            else:
                acc[:, where] = value

    sets = ((ee0, eo0, od0), (ee1, eo1, od1))
    products(0, *sets[0])
    for s in range(steps):
        if s + 1 < steps:
            products(s + 1, *sets[(s + 1) % 2])
        multiply(s, *sets[s % 2])

    table_loads[3].wait()
    own = lax.broadcasted_iota(jnp.int32, (1, RAD * 4 * nv), 1) % nv

    def place(v, carry):
        for h in range(2):
            two = [jnp.where(own == 2 * v + u, xv[h], 0.0) for u in range(2)]
            at = pl.multiple_of(h * height + v * 2 * planes, 16)
            xmat[pl.ds(at, 2 * planes), :] = jnp.concatenate(two, 0).astype(bf16)
        return carry

    lax.fori_loop(0, nv // 2, place, 0)

    lane = lax.broadcasted_iota(jnp.int32, (1, lanes), 1)
    occupied = jnp.zeros((1, lanes), jnp.int32)
    energy = jnp.zeros((1, lanes), f32)
    for v in range(nv):
        occupied = jnp.where(lane % nv == v, occ[v], occupied)
        energy = jnp.where(lane % nv == v, val_e[v], energy)
    factors = [
        jnp.sqrt(occupied.astype(f32) / (4.0 * (cond_e[me * bands + b] - energy)))
        * (1.0 / N**1.5)
        for b in range(bands)
    ]
    lower = lane < half
    groups = (
        (acc_e, 0, 128, TALL[0], ROWS[0], STARTS[0]),
        (acc_e, 256, 128, TALL[1], ROWS[1], STARTS[1]),
        (acc_o, 0, 256, TALL[2], ROWS[2], STARTS[2]),
    )
    for acc, base, w, tall, size, start in groups:
        summed = []
        for b in range(bands):
            at = slice(b * height, (b + 1) * height)
            turned = [
                acc[at, base + h * w : base + (h + 1) * w].astype(bf16).T[0:tall] for h in range(2)
            ]
            summed.append(
                jnp.dot(jnp.concatenate(turned, 1), xmat[...], preferred_element_type=f32)
            )
        for t in range(RAD // 2):
            first, second = [
                summed[b][0:size, t * lanes : (t + 1) * lanes] * factors[b] for b in range(bands)
            ]
            second = pltpu.roll(second, half, 1)
            at = 2 * t * NR + start
            sec[at : at + size, :] = jnp.where(lower, first, second)
            sec[at + NR : at + NR + size, :] = jnp.where(lower, second, first)

    index_copy.wait()
    pl.semaphore_wait(barrier, 1 + 3 * (count - 1))

    def pick(n):
        for u in range(PIECE):
            got[u : u + 1, :] = sec[pl.ds(idx[0, n * PIECE + u], 1), :]
        turned = got[...].T
        at = slice(n * PIECE, (n + 1) * PIECE)
        odd = ((gvec[0:1, at] - 1) & 1) == 1
        flip = gvec[1:2, at] < 0
        top, bottom = turned[0:half], turned[half:lanes]
        for b, both in enumerate((jnp.where(odd, bottom, top), jnp.where(odd, top, bottom))):
            chosen = jnp.where(flip, both[2 * nv : 4 * nv], both[0 : 2 * nv]).astype(bf16)
            part[n, b * nv : (b + 1) * nv, :] = chosen[0:nv]
            part[n, pairs + b * nv : pairs + (b + 1) * nv, :] = chosen[nv : 2 * nv]

    def right_copy(src, t):
        return remote(
            src.at[t], rin.at[t], chain_send.at[0, t], chain_recv.at[0, t],
            (p, jnp.minimum(g + 1, count - 1), c),
        )

    def left_copy(src, t):
        return remote(
            src.at[t], lin.at[t], chain_send.at[1, t], chain_recv.at[1, t],
            (p, jnp.maximum(g - 1, 0), c),
        )

    def chain(t, make, came, passed, first, last):
        @pl.when((t >= 0) & (t < pieces))
        def _():
            @pl.when(first)
            def _():
                make(part, t).start()

            @pl.when(jnp.logical_not(first))
            def _():
                make(part, t).wait_recv()

                @pl.when(jnp.logical_not(last))
                def _():
                    passed[t] = (part[t].astype(f32) + came[t].astype(f32)).astype(bf16)
                    make(passed, t).start()

    def row_copy(t, r, b, d, lo, wide, to):
        return remote(
            tot.at[t, pl.ds(r * pairs, pairs), pl.ds(lo, wide)],
            rows.at[me, :, pl.ds(to, wide)],
            row_send.at[t, r, d], row_recv.at[me], (b, g, d),
        )

    def put(t, r, b, d, lo, wide, to):
        here = (b == p) & (d == c)

        @pl.when(here)
        def _():
            rows[me, :, pl.ds(to, wide)] = tot[t, r * pairs : (r + 1) * pairs, lo : lo + wide]

        @pl.when(jnp.logical_not(here))
        def _():
            row_copy(t, r, b, d, lo, wide, to).start()

    def col_copy(t, r, j, k):
        at = pl.ds(pl.multiple_of(j * PIECE, 128), PIECE)
        return remote(
            tot.at[t, pl.ds(r * pairs, pairs), :], cols.at[me, :, at],
            col_send.at[j, k - 1], col_recv.at[p], (turn(p, k), g, c),
        )

    def finish(t):
        @pl.when((t >= 0) & (t < pieces))
        def _():
            mine = lambda: part[t].astype(f32)

            @pl.when(g == 0)
            def _():
                tot[t] = (mine() + lin[t].astype(f32)).astype(bf16)

            @pl.when(g == count - 1)
            def _():
                tot[t] = (mine() + rin[t].astype(f32)).astype(bf16)

            @pl.when((g > 0) & (g < count - 1))
            def _():
                tot[t] = (mine() + rin[t].astype(f32) + lin[t].astype(f32)).astype(bf16)

            h = t // per
            j = t - h * per
            for r in range(2):
                b = h + r * (count // 2)

                @pl.when(j < middle)
                def _():
                    put(t, r, b, 0, 0, PIECE, pl.multiple_of(j * PIECE, 128))

                @pl.when(j > middle)
                def _():
                    put(t, r, b, 1, 0, PIECE, pl.multiple_of(j * PIECE - low, 128))

                @pl.when(j == middle)
                def _():
                    put(t, r, b, 0, 0, span - middle * PIECE, middle * PIECE)
                    put(t, r, b, 1, low - middle * PIECE, (middle + 1) * PIECE - low, 0)

                @pl.when(b == g)
                def _():
                    at = pl.ds(pl.multiple_of(j * PIECE, 128), PIECE)
                    cols[me, :, at] = tot[t, r * pairs : (r + 1) * pairs, :]
                    for k in range(1, count):
                        col_copy(t, r, j, k).start()

    for n in range(pieces + LAG * (count - 1)):
        if n < pieces:
            pick(n)
        to_right = n - g * LAG
        to_left = n - (count - 1 - g) * LAG
        chain(to_right, right_copy, rin, rout, g == 0, g == count - 1)
        chain(to_left, left_copy, lin, lout, g == count - 1, g == 0)
        finish(jnp.minimum(to_right, to_left))

    def over(q, core):
        slot = q * 2 + core
        return remote(
            cols.at[slot], cols.at[slot], over_send.at[q], over_recv.at[q], (p, g, 1 - c)
        )

    def out_copy(ref, dst, slot, which):
        return pltpu.make_async_copy(ref.at[slot], dst.at[slot], outs.at[1 + which * slots + slot])

    over(p, c).start()
    out_copy(cols, cols_out, me, 0).start()
    for k in range(1, count):
        q = turn(p, k)
        at = q * 2 + c
        remote(cols.at[at], cols.at[at], col_send.at[0, 0], col_recv.at[q], (q, g, c)).wait_recv()
        over(q, c).start()
        out_copy(cols, cols_out, at, 0).start()
    for slot in range(slots):
        @pl.when(slot != me)
        def _():
            remote(
                rows.at[slot], rows.at[slot], row_send.at[0, 0, 0], row_recv.at[slot],
                (slot // 2, g, slot % 2),
            ).wait_recv()

        out_copy(rows, rows_out, slot, 1).start()
    for k in range(count):
        q = turn(p, k)
        over(q, 1 - c).wait_recv()
        out_copy(cols, cols_out, q * 2 + 1 - c, 0).start()

    for t in range(pieces):
        @pl.when(g < count - 1)
        def _():
            right_copy(part, t).wait_send()

        @pl.when(g > 0)
        def _():
            left_copy(part, t).wait_send()

        h, j = t // per, t % per
        for r in range(2):
            b = h + r * (count // 2)
            for d in range(2):
                if (j < middle and d == 1) or (j > middle and d == 0):
                    continue
                wide = PIECE
                if j == middle:
                    wide = (middle + 1) * PIECE - low if d else span - middle * PIECE

                @pl.when(jnp.logical_not((p == b) & (c == d)))
                def _():
                    row_copy(t, r, b, d, 0, wide, 0).wait_send()

            @pl.when(g == b)
            def _():
                for k in range(1, count):
                    col_copy(t, r, j, k).wait_send()

    for q in range(count):
        over(q, c).wait_send()
    for slot in range(slots):
        out_copy(cols, cols_out, slot, 0).wait()
        out_copy(rows, rows_out, slot, 1).wait()


def product_kernel(prefactor, rows, cols, out, turned):
    share = out.shape[0]
    c = lax.axis_index("gcol")
    shift = rows.shape[1] - share

    @pl.when(pl.program_id(0) == 0)
    def _():
        turned[...] = rows[...].T

    left = turned[pl.ds(pl.multiple_of(c * shift, 16), share), :]
    out[...] = jnp.dot(left, cols[...], preferred_element_type=jnp.float32) * prefactor


def product(rows, cols, share, prefactor):
    depth, width = cols.shape
    span = rows.shape[1]
    tile = 384
    return pl.pallas_call(
        functools.partial(product_kernel, prefactor),
        out_shape=jax.ShapeDtypeStruct((share, width), jnp.float32),
        grid=(width // tile,),
        in_specs=[
            pl.BlockSpec((depth, span), lambda i: (0, 0)),
            pl.BlockSpec((depth, tile), lambda i: (0, i)),
        ],
        out_specs=pl.BlockSpec((share, tile), lambda i: (0, i)),
        scratch_shapes=[pltpu.VMEM((span, depth), jnp.bfloat16)],
    )(rows, cols)


def fast_body(valence, conduction, val_energy, cond_energy, val_occupation, gvectors):
    nv, planes, points = valence.shape
    bands = conduction.shape[0]
    count = lax.axis_size("pair")
    gcol_count = lax.axis_size("gcol")
    height = nv * planes
    steps = QUARTER // STEP
    pairs = bands * nv
    width = 2 * KG // count
    slots = count * gcol_count
    pieces = KG // PIECE
    share = width // gcol_count
    span = width - share // 128 * 128
    bf16, f32 = jnp.bfloat16, jnp.float32
    left, right, sign = half_plane_tables()
    xtab = plane_table(nv)
    smem = pl.BlockSpec(memory_space=pltpu.SMEM)
    hbm = pl.BlockSpec(memory_space=pl.ANY)
    dma = pltpu.SemaphoreType.DMA
    piece = pltpu.VMEM((pieces, 2 * pairs, PIECE), bf16)
    chunk = [
        pltpu.VMEM((bands * height, STEP), bf16),
        pltpu.VMEM((bands * height, STEP), bf16),
        pltpu.VMEM((bands * height, 2 * STEP), bf16),
    ]
    cols, rows = pl.pallas_call(
        chi_kernel,
        out_shape=(
            jax.ShapeDtypeStruct((slots, pairs, width), bf16),
            jax.ShapeDtypeStruct((slots, pairs, span), bf16),
        ),
        in_specs=[smem] * 3 + [pl.BlockSpec(memory_space=pltpu.VMEM)] + [hbm] * 6,
        out_specs=(hbm, hbm),
        scratch_shapes=[
            pltpu.VMEM((nv, planes, points), bf16),
            pltpu.VMEM((bands, planes, points), bf16),
            pltpu.VMEM(left.shape, f32),
            pltpu.VMEM(right.shape, f32),
            pltpu.VMEM(sign.shape, f32),
            pltpu.VMEM((2, planes, RAD * 4 * nv), f32),
            pltpu.VMEM((QUARTER, 512), bf16),
            pltpu.VMEM((steps, 2 * STEP, 512), bf16),
            *chunk,
            *chunk,
            pltpu.VMEM((bands * height, 512), f32),
            pltpu.VMEM((bands * height, 512), f32),
            pltpu.VMEM((2 * height, RAD * 4 * nv), bf16),
            pltpu.VMEM((RAD * NR, 128), f32),
            pltpu.VMEM((PIECE, 128), f32),
            piece, piece, piece, piece, piece, piece,
            pltpu.VMEM((slots, pairs, width), bf16),
            pltpu.VMEM((slots, pairs, span), bf16),
            pltpu.VMEM((1, KG), jnp.int32),
            pltpu.SMEM((1, KG), jnp.int32),
            dma((8 * steps + 4,)),
            dma((2, pieces)),
            dma((2, pieces)),
            dma((pieces, 2, 2)),
            dma((slots,)),
            dma((width // PIECE, count - 1)),
            dma((count,)),
            dma((count,)),
            dma((count,)),
            dma((1 + 2 * slots,)),
        ],
        compiler_params=pltpu.CompilerParams(
            vmem_limit_bytes=60 * 1024 * 1024, collective_id=0, has_side_effects=True
        ),
    )(
        val_occupation, val_energy, cond_energy, gvectors,
        valence, conduction, left, right, sign, xtab,
    )
    all_pairs = slots * pairs
    prefactor = -1.0 / math.sqrt(all_pairs)
    return product(
        rows.reshape(all_pairs, span), cols.reshape(all_pairs, width), share, prefactor
    )


def either_body(valence, conduction, *rest):
    nv, planes, _ = valence.shape
    count = lax.axis_size("pair")
    width = 2 * KG // count
    fits = (
        count == lax.axis_size("grow")
        and count % 2 == 0
        and lax.axis_size("gcol") == 2
        and planes % 8 == 0
        and conduction.shape[0] == 2
        and 8 * nv == 128
        and width % PIECE == 0
        and width // PIECE % 2 == 1
    )
    return (fast_body if fits else body)(valence, conduction, *rest)


def solution(mesh):
    return jax.shard_map(
        either_body,
        mesh=mesh,
        in_specs=(P(None, "grow", None), P(("pair", "gcol"), "grow", None), P(), P(), P(), P()),
        out_specs=P(("pair", "gcol"), "grow"),
        check_vma=False,
    )
```

```python
import functools
import math

import jax
import jax.numpy as jnp
import numpy as np
from jax import lax
from jax.experimental import pallas as pl
from jax.experimental.pallas import tpu as pltpu
from jax.sharding import PartitionSpec as P

N = 96
RAD = 12
KG = 3840
NV = 16


def wave_tables(positions, frequencies):
    phases = jnp.mod(positions[:, None] * frequencies[None, :], N).astype(jnp.float32) * (
        2.0 * math.pi / N
    )
    return (jnp.cos(phases), jnp.sin(phases))


def build_tables(x_positions):
    all_freq = jnp.arange(-RAD, RAD + 1, dtype=jnp.int32)
    pos_freq = jnp.arange(1, RAD + 1, dtype=jnp.int32)
    positions = jnp.arange(N, dtype=jnp.int32)
    cosine, sine_part = wave_tables(positions, all_freq)
    z_table = jnp.concatenate([cosine, sine_part], 1).astype(jnp.bfloat16)
    y_table = jnp.stack(
        [jnp.stack([cosine, sine_part], 1), jnp.stack([-sine_part, cosine], 1)], 1
    ).astype(jnp.bfloat16)
    x_cos, x_sin = wave_tables(x_positions, pos_freq)
    x_table = jnp.stack([jnp.stack([x_cos, -x_sin], 1), jnp.stack([-x_sin, -x_cos], 1)], 1).astype(
        jnp.bfloat16
    )
    return (z_table, y_table, x_table)


def pair_product(left_rows, right_rows):
    return lax.dot_general(
        left_rows, right_rows, (((0,), (0,)), ((), ())), preferred_element_type=jnp.float32
    )


def body(valence, conduction, val_energy, cond_energy, val_occupation, gvectors):
    pair_count = lax.axis_size("pair")
    gcol_count = lax.axis_size("gcol")
    planes = valence.shape[1]
    cond_bands = conduction.shape[0]
    extent = 2 * RAD + 1
    local_pairs = cond_bands * NV
    x_positions = lax.axis_index("grow") * planes + jnp.arange(planes, dtype=jnp.int32)
    z_table, y_table, x_table = build_tables(x_positions)
    flat_index = ((gvectors[0] - 1) * extent + gvectors[1] + RAD) * extent + gvectors[2] + RAD
    density = conduction[:, None] * valence[None]
    section_one = jnp.dot(
        density.reshape(-1, N), z_table, preferred_element_type=jnp.float32
    ).astype(jnp.bfloat16)
    section_one = section_one.reshape(local_pairs * planes, N, 2, extent)
    second = jnp.einsum(
        "ayik,yioj->aojk", section_one, y_table, preferred_element_type=jnp.float32
    ).astype(jnp.bfloat16)
    second = second.reshape(local_pairs, planes, 2, extent * extent)
    section_three = jnp.einsum(
        "pxoq,xosm->psmq", second, x_table, preferred_element_type=jnp.float32
    )
    section_three = section_three.reshape(local_pairs, 2, RAD * extent * extent)
    picked = jnp.take(section_three, flat_index, axis=2).reshape(local_pairs, 2 * KG)
    summed = lax.psum_scatter(
        picked.astype(jnp.bfloat16), "grow", scatter_dimension=1, tiled=True
    ).astype(jnp.float32)
    first_band = (lax.axis_index("pair") * gcol_count + lax.axis_index("gcol")) * cond_bands
    own_energy = lax.dynamic_slice_in_dim(cond_energy, first_band, cond_bands, 0)
    weight = val_occupation.astype(jnp.float32)[None, :] / (
        4.0 * (own_energy[:, None] - val_energy[None, :])
    )
    factor = (jnp.sqrt(weight) * (1.0 / N**1.5)).reshape(local_pairs, 1)
    weighted = (summed * factor).astype(jnp.bfloat16)
    prefactor = -1.0 / math.sqrt(pair_count * gcol_count * local_pairs)
    full_rows = lax.all_gather(weighted, "grow", axis=1, tiled=True)
    row_part = lax.all_to_all(full_rows, "pair", split_axis=1, concat_axis=0, tiled=True)
    partial_value = pair_product(row_part, lax.all_gather(weighted, "pair", axis=0, tiled=True))
    return lax.psum_scatter(
        (partial_value * prefactor).astype(jnp.bfloat16), "gcol", scatter_dimension=0, tiled=True
    ).astype(jnp.float32)


EXT = 2 * RAD + 1
QUARTER = N * N // 4
STEP = 8 * N
TILE = 256
CLASSES = ((0, 4, 8, 12), (2, 6, 10), (1, 3, 5, 7, 9, 11))
WIDTHS = (128, 128, 256)
ROWS = (104, 80, 152)
STARTS = (0, 104, 184)
NR = 336
TALL = (112, 80, 160)
PIECE = 128
UNIT = 2
LAG = 4


def half_plane_tables():
    total = 2 * sum(WIDTHS)
    left = np.zeros((2, N // 4, total), np.float32)
    right = np.zeros((2, N, total), np.float32)
    sign = np.zeros((1, WIDTHS[2]), np.float32)
    y = np.arange(N // 4)[:, None]
    z = np.arange(N)[:, None]
    k = np.arange(-RAD, RAD + 1)
    base = 0
    for freqs, width in zip(CLASSES, WIDTHS):
        jj = np.repeat(np.array(freqs), EXT)[None]
        kk = np.tile(k, len(freqs))[None]
        count = jj.shape[1]
        ay = 2 * np.pi * ((jj * y) % N) / N
        az = 2 * np.pi * ((kk * z) % N) / N
        for part in range(2):
            cols = slice(base + part * width, base + part * width + count)
            left[0, :, cols] = np.sin(ay) if part else np.cos(ay)
            left[1, :, cols] = np.cos(ay) if part else -np.sin(ay)
            right[0, :, cols] = np.cos(az)
            right[1, :, cols] = np.sin(az)
        base += 2 * width
    jj = np.repeat(np.array(CLASSES[2]), EXT)
    sign[0, : jj.size] = np.where(jj % 4 == 1, 1.0, -1.0)
    return left, right, sign


def plane_table(pairs):
    x = np.arange(N)[:, None]
    a = np.arange(1, RAD + 1)[None]
    ang = 2 * np.pi * ((a * x) % N) / N
    c, s = np.cos(ang), np.sin(ang)
    tab = np.stack([np.stack([c, -s, c, -s], -1), np.stack([-s, -c, s, c], -1)])
    return np.repeat(tab.reshape(2, N, RAD * 4), pairs, axis=2).astype(np.float32)


def row_index(a, b, d):
    j = jnp.abs(b)
    k = jnp.where(b < 0, -d, d) + RAD
    row = jnp.where(
        (j & 1) == 1,
        STARTS[2] + (j >> 1) * EXT,
        jnp.where((j & 3) == 2, STARTS[1], STARTS[0]) + (j >> 2) * EXT,
    )
    return jnp.maximum((a - 1) * NR + row + k, 0)


def chi_kernel(
    occ, val_e, cond_e, gvec, val, cond, left, right, sign, xtab,
    cols_out, rows_out,
    orbitals, leftv, rightv, signv, xv, tabs, folded, acc, xmat, sec, got,
    part, rin, lin, rout, lout, tot, cols, rows, index, idx,
    loads, chain_send, chain_recv, row_send, row_recv, col_send, col_recv,
    over_send, over_recv, outs,
):
    f32, bf16 = jnp.float32, jnp.bfloat16
    nv, planes, _ = val.shape
    bands = cond.shape[0]
    height = nv * planes
    pairs = bands * nv
    lanes = 128
    half = lanes // 2
    steps = QUARTER // STEP
    pieces = part.shape[0]
    units = pieces // UNIT
    slots, _, width = cols.shape
    count = slots // 2
    per = width // PIECE
    middle = per // 2
    span = rows.shape[2]
    p, g, c = lax.axis_index("pair"), lax.axis_index("grow"), lax.axis_index("gcol")
    me = p * 2 + c
    turn = lambda at, k: lax.rem(at + k, count)

    def remote(src, dst, send, recv, to):
        return pltpu.make_async_remote_copy(
            src_ref=src, dst_ref=dst, send_sem=send, recv_sem=recv,
            device_id=to, device_id_type=pl.DeviceIdType.MESH,
        )

    table_loads = [
        pltpu.make_async_copy(a, b, loads.at[steps + i])
        for i, (a, b) in enumerate(
            (
                (left, leftv),
                (right, rightv),
                (sign, signv),
                (xtab.at[:, pl.ds(pl.multiple_of(g * planes, 8), planes), :], xv),
            )
        )
    ]
    step_loads = []
    for s in range(steps):
        group = []
        for q in range(4):
            at = pl.ds(q * QUARTER + s * STEP, STEP)
            for a, first in ((cond, nv), (val, 0)):
                b = orbitals.at[pl.ds(first, a.shape[0]), :, at]
                group.append(pltpu.make_async_copy(a.at[:, :, at], b, loads.at[s]))
        step_loads.append(group)
    for copy in table_loads[:3] + sum(step_loads, []) + table_loads[3:]:
        copy.start()

    barrier = pltpu.get_barrier_semaphore()
    pl.semaphore_signal(barrier, inc=1, device_id=(p, g, 1 - c))
    for k in range(1, count):
        for d in range(2):
            pl.semaphore_signal(barrier, inc=1, device_id=(turn(p, k), g, d))
        pl.semaphore_signal(barrier, inc=1, device_id=(p, turn(g, k), c))

    index[...] = row_index(gvec[0:1, :], gvec[1:2, :], gvec[2:3, :])
    index_copy = pltpu.make_async_copy(index, idx, outs.at[0])
    index_copy.start()

    for copy in table_loads[:3]:
        copy.wait()

    def table_rows(y, carry):
        l1, l2 = leftv[0, pl.ds(y, 1), :], leftv[1, pl.ds(y, 1), :]
        at = pl.ds(pl.multiple_of(y * N, 32), N)
        full = l1 * rightv[0] + l2 * rightv[1]
        odd_p, odd_q = full[:, 2 * TILE : 3 * TILE], full[:, 3 * TILE :]
        tiles = (
            full[:, 0:TILE], full[:, TILE : 2 * TILE],
            odd_p, odd_q * (0.0 - signv[...]), odd_q, odd_p * signv[...],
        )
        for i, tile in enumerate(tiles):
            tabs[i, at, :] = tile.astype(bf16)
        return carry

    lax.fori_loop(0, QUARTER // N, table_rows, 0)

    def ready(s):
        whole = orbitals.at[:, :, pl.ds(0, 4 * STEP)]
        pltpu.make_async_copy(whole, whole, loads.at[s]).wait()

    def products(i, carry):
        at = [pl.ds(pl.multiple_of(q * QUARTER + i * TILE, TILE), TILE) for q in range(4)]
        here = pl.ds(pl.multiple_of(i * TILE, TILE), TILE)
        for b in range(bands):
            for x in range(0, planes, 8):
                cs = [orbitals[nv + b, x : x + 8, q] for q in at]
                for v in range(nv):
                    d0, d1, d2, d3 = [orbitals[v, x : x + 8, q] * u for q, u in zip(at, cs)]
                    e0, e1 = d0 + d2, d1 + d3
                    row = b * height + v * planes + x
                    where = slice(row, row + 8)
                    folded[0, where, here] = e0 + e1
                    folded[1, where, here] = e0 - e1
                    folded[2, where, here] = d0 - d2
                    folded[3, where, here] = d1 - d3
        return carry

    for s in range(steps):
        ready(s)
        lax.fori_loop(s * STEP // TILE, (s + 1) * STEP // TILE, products, 0)

    dot = lambda i, j: jnp.dot(folded[i], tabs[j], preferred_element_type=f32)
    acc[0] = dot(0, 0)
    acc[1] = dot(1, 1)
    acc[2] = dot(2, 2) + dot(3, 3)
    acc[3] = dot(2, 4) + dot(3, 5)

    table_loads[3].wait()
    own = lax.broadcasted_iota(jnp.int32, (1, RAD * 4 * nv), 1) % nv

    def place(v, carry):
        for h in range(2):
            two = [jnp.where(own == 2 * v + u, xv[h], 0.0) for u in range(2)]
            at = pl.multiple_of(h * height + v * 2 * planes, 16)
            xmat[pl.ds(at, 2 * planes), :] = jnp.concatenate(two, 0).astype(bf16)
        return carry

    lax.fori_loop(0, nv // 2, place, 0)

    lane = lax.broadcasted_iota(jnp.int32, (1, lanes), 1)
    occupied = jnp.zeros((1, lanes), jnp.int32)
    energy = jnp.zeros((1, lanes), f32)
    for v in range(nv):
        occupied = jnp.where(lane % nv == v, occ[v], occupied)
        energy = jnp.where(lane % nv == v, val_e[v], energy)
    factors = [
        jnp.sqrt(occupied.astype(f32) / (4.0 * (cond_e[me * bands + b] - energy)))
        * (1.0 / N**1.5)
        for b in range(bands)
    ]
    lower = lane < half
    groups = (
        ((0,), (0,), (0, 128), 128, TALL[0], ROWS[0], STARTS[0]),
        ((1,), (1,), (0, 128), 128, TALL[1], ROWS[1], STARTS[1]),
        ((2,), (3,), (0, 0), 256, TALL[2], ROWS[2], STARTS[2]),
    )
    for first_of, second_of, bases, size_of, tall, size, start in groups:
        summed = []
        for b in range(bands):
            at = slice(b * height, (b + 1) * height)
            turned = [
                sum(acc[i, at, base : base + size_of] for i in which).astype(bf16).T[0:tall]
                for which, base in zip((first_of, second_of), bases)
            ]
            summed.append(
                jnp.dot(jnp.concatenate(turned, 1), xmat[...], preferred_element_type=f32)
            )
        for t in range(RAD // 2):
            first, second = [
                summed[b][0:size, t * lanes : (t + 1) * lanes] * factors[b] for b in range(bands)
            ]
            second = pltpu.roll(second, half, 1)
            at = 2 * t * NR + start
            sec[at : at + size, :] = jnp.where(lower, first, second)
            sec[at + NR : at + NR + size, :] = jnp.where(lower, second, first)

    index_copy.wait()
    pl.semaphore_wait(barrier, 1 + 3 * (count - 1))

    def pick(n):
        at = pl.ds(pl.multiple_of(n * PIECE, PIECE), PIECE)
        for u in range(PIECE):
            got[u : u + 1, :] = sec[pl.ds(idx[0, n * PIECE + u], 1), :]
        turned = got[...].T
        odd = ((gvec[0:1, at] - 1) & 1) == 1
        flip = gvec[1:2, at] < 0
        top, bottom = turned[0:half], turned[half:lanes]
        for b, both in enumerate((jnp.where(odd, bottom, top), jnp.where(odd, top, bottom))):
            chosen = jnp.where(flip, both[2 * nv : 4 * nv], both[0 : 2 * nv]).astype(bf16)
            part[n, b * nv : (b + 1) * nv, :] = chosen[0:nv]
            part[n, pairs + b * nv : pairs + (b + 1) * nv, :] = chosen[nv : 2 * nv]

    def right_copy(src, t):
        at = pl.ds(t * UNIT, UNIT)
        return remote(
            src.at[at], rin.at[at], chain_send.at[0], chain_recv.at[0, t],
            (p, jnp.minimum(g + 1, count - 1), c),
        )

    def left_copy(src, t):
        at = pl.ds(t * UNIT, UNIT)
        return remote(
            src.at[at], lin.at[at], chain_send.at[1], chain_recv.at[1, t],
            (p, jnp.maximum(g - 1, 0), c),
        )

    def chain(t, make, came, passed, first, last):
        @pl.when((t >= 0) & (t < units))
        def _():
            @pl.when(first)
            def _():
                make(part, t).start()

            @pl.when(jnp.logical_not(first))
            def _():
                make(part, t).wait_recv()

                @pl.when(jnp.logical_not(last))
                def _():
                    at = pl.ds(t * UNIT, UNIT)
                    passed[at] = (part[at].astype(f32) + came[at].astype(f32)).astype(bf16)
                    make(passed, t).start()

    def row_copy(t, r, b, d, j):
        at = pl.ds(pl.multiple_of(j * PIECE, PIECE), PIECE)
        return remote(
            tot.at[t, pl.ds(r * pairs, pairs), :], rows.at[me, :, at],
            row_send.at[0], row_recv.at[me], (b, g, d),
        )

    def put(t, r, b, d, j):
        here = (b == p) & (d == c)

        @pl.when(here)
        def _():
            at = pl.ds(pl.multiple_of(j * PIECE, PIECE), PIECE)
            rows[me, :, at] = tot[t, r * pairs : (r + 1) * pairs, :]

        @pl.when(jnp.logical_not(here))
        def _():
            row_copy(t, r, b, d, j).start()

    def col_copy(t, r, j, k):
        at = pl.ds(pl.multiple_of(j * PIECE, 128), PIECE)
        return remote(
            tot.at[t, pl.ds(r * pairs, pairs), :], cols.at[me, :, at],
            col_send.at[0], col_recv.at[p], (turn(p, k), g, c),
        )

    def deliver(t):
        h = t // per
        j = t - h * per
        for r in range(2):
            b = h + r * (count // 2)

            @pl.when(j <= middle)
            def _():
                put(t, r, b, 0, j)

            @pl.when(j >= middle)
            def _():
                put(t, r, b, 1, j - middle)

            @pl.when(b == g)
            def _():
                at = pl.ds(pl.multiple_of(j * PIECE, 128), PIECE)
                cols[me, :, at] = tot[t, r * pairs : (r + 1) * pairs, :]
                for k in range(1, count):
                    col_copy(t, r, j, k).start()

    def finish(u):
        @pl.when((u >= 0) & (u < units))
        def _():
            at = pl.ds(u * UNIT, UNIT)
            mine = lambda: part[at].astype(f32)

            @pl.when(g == 0)
            def _():
                tot[at] = (mine() + lin[at].astype(f32)).astype(bf16)

            @pl.when(g == count - 1)
            def _():
                tot[at] = (mine() + rin[at].astype(f32)).astype(bf16)

            @pl.when((g > 0) & (g < count - 1))
            def _():
                tot[at] = (mine() + rin[at].astype(f32) + lin[at].astype(f32)).astype(bf16)

            for i in range(UNIT):
                deliver(u * UNIT + i)

    def serve(n):
        to_right = n - g * LAG
        to_left = n - (count - 1 - g) * LAG
        chain(to_right, right_copy, rin, rout, g == 0, g == count - 1)
        chain(to_left, left_copy, lin, lout, g == count - 1, g == 0)
        finish(jnp.minimum(to_right, to_left))

    def early(n, carry):
        for i in range(UNIT):
            pick(n * UNIT + i)
        serve(n)
        return carry

    def late(n, carry):
        serve(n)
        return carry

    lax.fori_loop(0, units, early, 0)
    lax.fori_loop(units, units + LAG * (count - 1), late, 0)

    def over(q, core):
        slot = q * 2 + core
        return remote(
            cols.at[slot], cols.at[slot], over_send.at[0], over_recv.at[q], (p, g, 1 - c)
        )

    def out_copy(ref, dst, slot, which):
        return pltpu.make_async_copy(ref.at[slot], dst.at[slot], outs.at[1 + which])

    over(p, c).start()
    out_copy(cols, cols_out, me, 0).start()
    for k in range(1, count):
        q = turn(p, k)
        at = q * 2 + c
        remote(cols.at[at], cols.at[at], col_send.at[0], col_recv.at[q], (q, g, c)).wait_recv()
        over(q, c).start()
        out_copy(cols, cols_out, at, 0).start()
    for slot in range(slots):
        @pl.when(slot != me)
        def _():
            remote(
                rows.at[slot], rows.at[slot], row_send.at[0], row_recv.at[slot],
                (slot // 2, g, slot % 2),
            ).wait_recv()

        out_copy(rows, rows_out, slot, 1).start()
    for k in range(count):
        q = turn(p, k)
        over(q, 1 - c).wait_recv()
        out_copy(cols, cols_out, q * 2 + 1 - c, 0).start()

    def sent(ref, sem):
        remote(ref, ref, sem, row_recv.at[0], (p, g, 1 - c)).wait_send()

    @pl.when(g < count - 1)
    def _():
        sent(part, chain_send.at[0])

    @pl.when(g > 0)
    def _():
        sent(part, chain_send.at[1])

    sent(rows.at[pl.ds(0, slots - 1)], row_send.at[0])
    sent(cols.at[pl.ds(0, count - 1)], col_send.at[0])
    sent(cols.at[pl.ds(0, count)], over_send.at[0])
    pltpu.make_async_copy(cols, cols_out, outs.at[1]).wait()
    pltpu.make_async_copy(rows, rows_out, outs.at[2]).wait()


def product_kernel(prefactor, rows, cols, out, turned):
    share = out.shape[0]
    c = lax.axis_index("gcol")
    shift = rows.shape[1] - share

    @pl.when(pl.program_id(0) == 0)
    def _():
        turned[...] = rows[...].T

    left = turned[pl.ds(pl.multiple_of(c * shift, 16), share), :]
    out[...] = jnp.dot(left, cols[...], preferred_element_type=jnp.float32) * prefactor


def product(rows, cols, share, prefactor):
    depth, width = cols.shape
    span = rows.shape[1]
    tile = 384
    return pl.pallas_call(
        functools.partial(product_kernel, prefactor),
        out_shape=jax.ShapeDtypeStruct((share, width), jnp.float32),
        grid=(width // tile,),
        in_specs=[
            pl.BlockSpec((depth, span), lambda i: (0, 0)),
            pl.BlockSpec((depth, tile), lambda i: (0, i)),
        ],
        out_specs=pl.BlockSpec((share, tile), lambda i: (0, i)),
        scratch_shapes=[pltpu.VMEM((span, depth), jnp.bfloat16)],
    )(rows, cols)


def fast_body(valence, conduction, val_energy, cond_energy, val_occupation, gvectors):
    nv, planes, points = valence.shape
    bands = conduction.shape[0]
    count = lax.axis_size("pair")
    gcol_count = lax.axis_size("gcol")
    height = nv * planes
    steps = QUARTER // STEP
    pairs = bands * nv
    width = 2 * KG // count
    slots = count * gcol_count
    pieces = KG // PIECE
    share = width // gcol_count
    span = width - share // 128 * 128
    bf16, f32 = jnp.bfloat16, jnp.float32
    left, right, sign = half_plane_tables()
    xtab = plane_table(nv)
    smem = pl.BlockSpec(memory_space=pltpu.SMEM)
    hbm = pl.BlockSpec(memory_space=pl.ANY)
    dma = pltpu.SemaphoreType.DMA
    piece = pltpu.VMEM((pieces, 2 * pairs, PIECE), bf16)
    cols, rows = pl.pallas_call(
        chi_kernel,
        out_shape=(
            jax.ShapeDtypeStruct((slots, pairs, width), bf16),
            jax.ShapeDtypeStruct((slots, pairs, span), bf16),
        ),
        in_specs=[smem] * 3 + [pl.BlockSpec(memory_space=pltpu.VMEM)] + [hbm] * 6,
        out_specs=(hbm, hbm),
        scratch_shapes=[
            pltpu.VMEM((nv + bands, planes, points), bf16),
            pltpu.VMEM(left.shape, f32),
            pltpu.VMEM(right.shape, f32),
            pltpu.VMEM(sign.shape, f32),
            pltpu.VMEM((2, planes, RAD * 4 * nv), f32),
            pltpu.VMEM((6, QUARTER, TILE), bf16),
            pltpu.VMEM((4, bands * height, QUARTER), bf16),
            pltpu.VMEM((4, bands * height, TILE), f32),
            pltpu.VMEM((2 * height, RAD * 4 * nv), bf16),
            pltpu.VMEM((RAD * NR, 128), f32),
            pltpu.VMEM((PIECE, 128), f32),
            piece, piece, piece, piece, piece, piece,
            pltpu.VMEM((slots, pairs, width), bf16),
            pltpu.VMEM((slots, pairs, span), bf16),
            pltpu.VMEM((1, KG), jnp.int32),
            pltpu.SMEM((1, KG), jnp.int32),
            dma((steps + 4,)),
            dma((2,)),
            dma((2, pieces // UNIT)),
            dma((1,)),
            dma((slots,)),
            dma((1,)),
            dma((count,)),
            dma((1,)),
            dma((count,)),
            dma((3,)),
        ],
        compiler_params=pltpu.CompilerParams(
            vmem_limit_bytes=60 * 1024 * 1024, collective_id=0, has_side_effects=True
        ),
    )(
        val_occupation, val_energy, cond_energy, gvectors,
        valence, conduction, left, right, sign, xtab,
    )
    all_pairs = slots * pairs
    prefactor = -1.0 / math.sqrt(all_pairs)
    return product(
        rows.reshape(all_pairs, span), cols.reshape(all_pairs, width), share, prefactor
    )


def either_body(valence, conduction, *rest):
    nv, planes, _ = valence.shape
    count = lax.axis_size("pair")
    width = 2 * KG // count
    fits = (
        count == lax.axis_size("grow")
        and count % 2 == 0
        and lax.axis_size("gcol") == 2
        and planes % 8 == 0
        and conduction.shape[0] == 2
        and 8 * nv == 128
        and width % PIECE == 0
        and width // PIECE % 2 == 1
        and KG // PIECE % UNIT == 0
    )
    return (fast_body if fits else body)(valence, conduction, *rest)


def solution(mesh):
    return jax.shard_map(
        either_body,
        mesh=mesh,
        in_specs=(P(None, "grow", None), P(("pair", "gcol"), "grow", None), P(), P(), P(), P()),
        out_specs=P(("pair", "gcol"), "grow"),
        check_vma=False,
    )
```

```python
import functools
import math

import jax
import jax.numpy as jnp
import numpy as np
from jax import lax
from jax.experimental import pallas as pl
from jax.experimental.pallas import tpu as pltpu
from jax.sharding import PartitionSpec as P

N = 96
RAD = 12
KG = 3840
NV = 16


def wave_tables(positions, frequencies):
    phases = jnp.mod(positions[:, None] * frequencies[None, :], N).astype(jnp.float32) * (
        2.0 * math.pi / N
    )
    return (jnp.cos(phases), jnp.sin(phases))


def build_tables(x_positions):
    all_freq = jnp.arange(-RAD, RAD + 1, dtype=jnp.int32)
    pos_freq = jnp.arange(1, RAD + 1, dtype=jnp.int32)
    positions = jnp.arange(N, dtype=jnp.int32)
    cosine, sine_part = wave_tables(positions, all_freq)
    z_table = jnp.concatenate([cosine, sine_part], 1).astype(jnp.bfloat16)
    y_table = jnp.stack(
        [jnp.stack([cosine, sine_part], 1), jnp.stack([-sine_part, cosine], 1)], 1
    ).astype(jnp.bfloat16)
    x_cos, x_sin = wave_tables(x_positions, pos_freq)
    x_table = jnp.stack([jnp.stack([x_cos, -x_sin], 1), jnp.stack([-x_sin, -x_cos], 1)], 1).astype(
        jnp.bfloat16
    )
    return (z_table, y_table, x_table)


def pair_product(left_rows, right_rows):
    return lax.dot_general(
        left_rows, right_rows, (((0,), (0,)), ((), ())), preferred_element_type=jnp.float32
    )


def body(valence, conduction, val_energy, cond_energy, val_occupation, gvectors):
    pair_count = lax.axis_size("pair")
    gcol_count = lax.axis_size("gcol")
    planes = valence.shape[1]
    cond_bands = conduction.shape[0]
    extent = 2 * RAD + 1
    local_pairs = cond_bands * NV
    x_positions = lax.axis_index("grow") * planes + jnp.arange(planes, dtype=jnp.int32)
    z_table, y_table, x_table = build_tables(x_positions)
    flat_index = ((gvectors[0] - 1) * extent + gvectors[1] + RAD) * extent + gvectors[2] + RAD
    density = conduction[:, None] * valence[None]
    section_one = jnp.dot(
        density.reshape(-1, N), z_table, preferred_element_type=jnp.float32
    ).astype(jnp.bfloat16)
    section_one = section_one.reshape(local_pairs * planes, N, 2, extent)
    second = jnp.einsum(
        "ayik,yioj->aojk", section_one, y_table, preferred_element_type=jnp.float32
    ).astype(jnp.bfloat16)
    second = second.reshape(local_pairs, planes, 2, extent * extent)
    section_three = jnp.einsum(
        "pxoq,xosm->psmq", second, x_table, preferred_element_type=jnp.float32
    )
    section_three = section_three.reshape(local_pairs, 2, RAD * extent * extent)
    picked = jnp.take(section_three, flat_index, axis=2).reshape(local_pairs, 2 * KG)
    summed = lax.psum_scatter(
        picked.astype(jnp.bfloat16), "grow", scatter_dimension=1, tiled=True
    ).astype(jnp.float32)
    first_band = (lax.axis_index("pair") * gcol_count + lax.axis_index("gcol")) * cond_bands
    own_energy = lax.dynamic_slice_in_dim(cond_energy, first_band, cond_bands, 0)
    weight = val_occupation.astype(jnp.float32)[None, :] / (
        4.0 * (own_energy[:, None] - val_energy[None, :])
    )
    factor = (jnp.sqrt(weight) * (1.0 / N**1.5)).reshape(local_pairs, 1)
    weighted = (summed * factor).astype(jnp.bfloat16)
    prefactor = -1.0 / math.sqrt(pair_count * gcol_count * local_pairs)
    full_rows = lax.all_gather(weighted, "grow", axis=1, tiled=True)
    row_part = lax.all_to_all(full_rows, "pair", split_axis=1, concat_axis=0, tiled=True)
    partial_value = pair_product(row_part, lax.all_gather(weighted, "pair", axis=0, tiled=True))
    return lax.psum_scatter(
        (partial_value * prefactor).astype(jnp.bfloat16), "gcol", scatter_dimension=0, tiled=True
    ).astype(jnp.float32)


EXT = 2 * RAD + 1
QUARTER = N * N // 4
STEP = 8 * N
TILE = 256
CLASSES = ((0, 4, 8, 12), (2, 6, 10), (1, 3, 5, 7, 9, 11))
WIDTHS = (128, 128, 256)
ROWS = (104, 80, 152)
STARTS = (0, 104, 184)
NR = 336
TALL = (112, 80, 160)
PIECE = 128
UNIT = 2
LAG = 4


def half_plane_tables():
    total = 2 * sum(WIDTHS)
    left = np.zeros((2, N // 4, total), np.float32)
    right = np.zeros((2, N, total), np.float32)
    sign = np.zeros((1, WIDTHS[2]), np.float32)
    y = np.arange(N // 4)[:, None]
    z = np.arange(N)[:, None]
    k = np.arange(-RAD, RAD + 1)
    base = 0
    for freqs, width in zip(CLASSES, WIDTHS):
        jj = np.repeat(np.array(freqs), EXT)[None]
        kk = np.tile(k, len(freqs))[None]
        count = jj.shape[1]
        ay = 2 * np.pi * ((jj * y) % N) / N
        az = 2 * np.pi * ((kk * z) % N) / N
        for part in range(2):
            cols = slice(base + part * width, base + part * width + count)
            left[0, :, cols] = np.sin(ay) if part else np.cos(ay)
            left[1, :, cols] = np.cos(ay) if part else -np.sin(ay)
            right[0, :, cols] = np.cos(az)
            right[1, :, cols] = np.sin(az)
        base += 2 * width
    jj = np.repeat(np.array(CLASSES[2]), EXT)
    sign[0, : jj.size] = np.where(jj % 4 == 1, 1.0, -1.0)
    return left, right, sign


def plane_table(pairs):
    x = np.arange(N)[:, None]
    a = np.arange(1, RAD + 1)[None]
    ang = 2 * np.pi * ((a * x) % N) / N
    c, s = np.cos(ang), np.sin(ang)
    tab = np.stack([np.stack([c, -s, c, -s], -1), np.stack([-s, -c, s, c], -1)])
    return np.repeat(tab.reshape(2, N, RAD * 4), pairs, axis=2).astype(np.float32)


def row_index(a, b, d):
    j = jnp.abs(b)
    k = jnp.where(b < 0, -d, d) + RAD
    row = jnp.where(
        (j & 1) == 1,
        STARTS[2] + (j >> 1) * EXT,
        jnp.where((j & 3) == 2, STARTS[1], STARTS[0]) + (j >> 2) * EXT,
    )
    return jnp.maximum((a - 1) * NR + row + k, 0)


def chi_kernel(
    occ_in, val_in, cond_in, gvec_in, val, cond, left, right, sign, xtab,
    cols, rows,
    occ, val_e, cond_e, gvec, orbitals, leftv, rightv, signv, xv, tabs, folded, acc, xmat, sec, got,
    part, rin, lin, rout, lout, tot, index, idx,
    loads, chain_send, chain_recv, row_send, row_recv, col_send, col_recv,
    over_send, over_recv, outs,
):
    f32, bf16 = jnp.float32, jnp.bfloat16
    nv, planes, _ = val.shape
    bands = cond.shape[0]
    height = nv * planes
    pairs = bands * nv
    lanes = 128
    half = lanes // 2
    steps = QUARTER // STEP
    pieces = part.shape[0]
    units = pieces // UNIT
    slots, _, width = cols.shape
    count = slots // 2
    per = width // PIECE
    middle = per // 2
    span = rows.shape[2]
    p, g, c = lax.axis_index("pair"), lax.axis_index("grow"), lax.axis_index("gcol")
    me = p * 2 + c
    turn = lambda at, k: lax.rem(at + k, count)

    def remote(src, dst, send, recv, to):
        return pltpu.make_async_remote_copy(
            src_ref=src, dst_ref=dst, send_sem=send, recv_sem=recv,
            device_id=to, device_id_type=pl.DeviceIdType.MESH,
        )

    table_loads = [
        pltpu.make_async_copy(a, b, loads.at[steps + i])
        for i, (a, b) in enumerate(
            (
                (left, leftv),
                (right, rightv),
                (sign, signv),
                (gvec_in, gvec),
                (xtab.at[:, pl.ds(pl.multiple_of(g * planes, 8), planes), :], xv),
                (occ_in, occ),
                (val_in, val_e),
                (cond_in, cond_e),
            )
        )
    ]
    step_loads = []
    for s in range(steps):
        group = []
        for q in range(4):
            at = pl.ds(q * QUARTER + s * STEP, STEP)
            for a, first in ((cond, nv), (val, 0)):
                b = orbitals.at[pl.ds(first, a.shape[0]), :, at]
                group.append(pltpu.make_async_copy(a.at[:, :, at], b, loads.at[s]))
        step_loads.append(group)
    for copy in table_loads[:4] + sum(step_loads, []) + table_loads[4:]:
        copy.start()

    barrier = pltpu.get_barrier_semaphore()
    pl.semaphore_signal(barrier, inc=1, device_id=(p, g, 1 - c))
    for k in range(1, count):
        for d in range(2):
            pl.semaphore_signal(barrier, inc=1, device_id=(turn(p, k), g, d))
        pl.semaphore_signal(barrier, inc=1, device_id=(p, turn(g, k), c))

    for copy in table_loads[:4]:
        copy.wait()
    index[...] = row_index(gvec[0:1, :], gvec[1:2, :], gvec[2:3, :])
    index_copy = pltpu.make_async_copy(index, idx, outs.at[0])
    index_copy.start()

    def table_rows(y, carry):
        l1, l2 = leftv[0, pl.ds(y, 1), :], leftv[1, pl.ds(y, 1), :]
        at = pl.ds(pl.multiple_of(y * N, 32), N)
        full = l1 * rightv[0] + l2 * rightv[1]
        odd_p, odd_q = full[:, 2 * TILE : 3 * TILE], full[:, 3 * TILE :]
        tiles = (
            full[:, 0:TILE], full[:, TILE : 2 * TILE],
            odd_p, odd_q * (0.0 - signv[...]), odd_q, odd_p * signv[...],
        )
        for i, tile in enumerate(tiles):
            tabs[i, at, :] = tile.astype(bf16)
        return carry

    lax.fori_loop(0, QUARTER // N, table_rows, 0)

    def ready(s):
        whole = orbitals.at[:, :, pl.ds(0, 4 * STEP)]
        pltpu.make_async_copy(whole, whole, loads.at[s]).wait()

    def products(i, carry):
        at = [pl.ds(pl.multiple_of(q * QUARTER + i * TILE, TILE), TILE) for q in range(4)]
        here = pl.ds(pl.multiple_of(i * TILE, TILE), TILE)
        for b in range(bands):
            for x in range(0, planes, 8):
                cs = [orbitals[nv + b, x : x + 8, q] for q in at]
                for v in range(nv):
                    d0, d1, d2, d3 = [orbitals[v, x : x + 8, q] * u for q, u in zip(at, cs)]
                    e0, e1 = d0 + d2, d1 + d3
                    row = b * height + v * planes + x
                    where = slice(row, row + 8)
                    folded[0, where, here] = e0 + e1
                    folded[1, where, here] = e0 - e1
                    folded[2, where, here] = d0 - d2
                    folded[3, where, here] = d1 - d3
        return carry

    for s in range(steps):
        ready(s)
        lax.fori_loop(s * STEP // TILE, (s + 1) * STEP // TILE, products, 0)

    dot = lambda i, j: jnp.dot(folded[i], tabs[j], preferred_element_type=f32)
    acc[0] = dot(0, 0)
    acc[1] = dot(1, 1)
    acc[2] = dot(2, 2) + dot(3, 3)
    acc[3] = dot(2, 4) + dot(3, 5)

    for copy in table_loads[4:]:
        copy.wait()
    own = lax.broadcasted_iota(jnp.int32, (1, RAD * 4 * nv), 1) % nv

    def place(v, carry):
        for h in range(2):
            two = [jnp.where(own == 2 * v + u, xv[h], 0.0) for u in range(2)]
            at = pl.multiple_of(h * height + v * 2 * planes, 16)
            xmat[pl.ds(at, 2 * planes), :] = jnp.concatenate(two, 0).astype(bf16)
        return carry

    lax.fori_loop(0, nv // 2, place, 0)

    lane = lax.broadcasted_iota(jnp.int32, (1, lanes), 1)
    occupied = jnp.zeros((1, lanes), jnp.int32)
    energy = jnp.zeros((1, lanes), f32)
    for v in range(nv):
        occupied = jnp.where(lane % nv == v, occ[v], occupied)
        energy = jnp.where(lane % nv == v, val_e[v], energy)
    factors = [
        jnp.sqrt(occupied.astype(f32) / (4.0 * (cond_e[me * bands + b] - energy)))
        * (1.0 / N**1.5)
        for b in range(bands)
    ]
    lower = lane < half
    groups = (
        ((0,), (0,), (0, 128), 128, TALL[0], ROWS[0], STARTS[0]),
        ((1,), (1,), (0, 128), 128, TALL[1], ROWS[1], STARTS[1]),
        ((2,), (3,), (0, 0), 256, TALL[2], ROWS[2], STARTS[2]),
    )
    for first_of, second_of, bases, size_of, tall, size, start in groups:
        summed = []
        for b in range(bands):
            at = slice(b * height, (b + 1) * height)
            turned = [
                sum(acc[i, at, base : base + size_of] for i in which).astype(bf16).T[0:tall]
                for which, base in zip((first_of, second_of), bases)
            ]
            summed.append(
                jnp.dot(jnp.concatenate(turned, 1), xmat[...], preferred_element_type=f32)
            )
        for t in range(RAD // 2):
            first, second = [
                summed[b][0:size, t * lanes : (t + 1) * lanes] * factors[b] for b in range(bands)
            ]
            second = pltpu.roll(second, half, 1)
            at = 2 * t * NR + start
            sec[at : at + size, :] = jnp.where(lower, first, second)
            sec[at + NR : at + NR + size, :] = jnp.where(lower, second, first)

    index_copy.wait()
    pl.semaphore_wait(barrier, 1 + 3 * (count - 1))

    def pick(n):
        at = pl.ds(pl.multiple_of(n * PIECE, PIECE), PIECE)
        for u in range(PIECE):
            got[u : u + 1, :] = sec[pl.ds(idx[0, n * PIECE + u], 1), :]
        turned = got[...].T
        odd = ((gvec[0:1, at] - 1) & 1) == 1
        flip = gvec[1:2, at] < 0
        top, bottom = turned[0:half], turned[half:lanes]
        for b, both in enumerate((jnp.where(odd, bottom, top), jnp.where(odd, top, bottom))):
            chosen = jnp.where(flip, both[2 * nv : 4 * nv], both[0 : 2 * nv]).astype(bf16)
            part[n, b * nv : (b + 1) * nv, :] = chosen[0:nv]
            part[n, pairs + b * nv : pairs + (b + 1) * nv, :] = chosen[nv : 2 * nv]

    def right_copy(src, t):
        at = pl.ds(t * UNIT, UNIT)
        return remote(
            src.at[at], rin.at[at], chain_send.at[0], chain_recv.at[0, t],
            (p, jnp.minimum(g + 1, count - 1), c),
        )

    def left_copy(src, t):
        at = pl.ds(t * UNIT, UNIT)
        return remote(
            src.at[at], lin.at[at], chain_send.at[1], chain_recv.at[1, t],
            (p, jnp.maximum(g - 1, 0), c),
        )

    def chain(t, make, came, passed, first, last):
        @pl.when((t >= 0) & (t < units))
        def _():
            @pl.when(first)
            def _():
                make(part, t).start()

            @pl.when(jnp.logical_not(first))
            def _():
                make(part, t).wait_recv()

                @pl.when(jnp.logical_not(last))
                def _():
                    at = pl.ds(t * UNIT, UNIT)
                    passed[at] = (part[at].astype(f32) + came[at].astype(f32)).astype(bf16)
                    make(passed, t).start()

    def row_copy(t, r, b, d, j):
        at = pl.ds(pl.multiple_of(j * PIECE, PIECE), PIECE)
        return remote(
            tot.at[t, pl.ds(r * pairs, pairs), :], rows.at[me, :, at],
            row_send.at[0], row_recv.at[me], (b, g, d),
        )

    def put(t, r, b, d, j):
        here = (b == p) & (d == c)

        @pl.when(here)
        def _():
            at = pl.ds(pl.multiple_of(j * PIECE, PIECE), PIECE)
            rows[me, :, at] = tot[t, r * pairs : (r + 1) * pairs, :]

        @pl.when(jnp.logical_not(here))
        def _():
            row_copy(t, r, b, d, j).start()

    def col_copy(t, r, j, k):
        at = pl.ds(pl.multiple_of(j * PIECE, 128), PIECE)
        return remote(
            tot.at[t, pl.ds(r * pairs, pairs), :], cols.at[me, :, at],
            col_send.at[0], col_recv.at[p], (turn(p, k), g, c),
        )

    def deliver(t):
        h = t // per
        j = t - h * per
        for r in range(2):
            b = h + r * (count // 2)

            @pl.when(j <= middle)
            def _():
                put(t, r, b, 0, j)

            @pl.when(j >= middle)
            def _():
                put(t, r, b, 1, j - middle)

            @pl.when(b == g)
            def _():
                at = pl.ds(pl.multiple_of(j * PIECE, 128), PIECE)
                cols[me, :, at] = tot[t, r * pairs : (r + 1) * pairs, :]
                for k in range(1, count):
                    col_copy(t, r, j, k).start()

    def finish(u):
        @pl.when((u >= 0) & (u < units))
        def _():
            at = pl.ds(u * UNIT, UNIT)
            mine = lambda: part[at].astype(f32)

            @pl.when(g == 0)
            def _():
                tot[at] = (mine() + lin[at].astype(f32)).astype(bf16)

            @pl.when(g == count - 1)
            def _():
                tot[at] = (mine() + rin[at].astype(f32)).astype(bf16)

            @pl.when((g > 0) & (g < count - 1))
            def _():
                tot[at] = (mine() + rin[at].astype(f32) + lin[at].astype(f32)).astype(bf16)

            for i in range(UNIT):
                deliver(u * UNIT + i)

    def serve(n):
        to_right = n - g * LAG
        to_left = n - (count - 1 - g) * LAG
        chain(to_right, right_copy, rin, rout, g == 0, g == count - 1)
        chain(to_left, left_copy, lin, lout, g == count - 1, g == 0)
        finish(jnp.minimum(to_right, to_left))

    def early(n, carry):
        for i in range(UNIT):
            pick(n * UNIT + i)
        serve(n)
        return carry

    def late(n, carry):
        serve(n)
        return carry

    lax.fori_loop(0, units, early, 0)
    lax.fori_loop(units, units + LAG * (count - 1), late, 0)

    def over(q, core):
        slot = q * 2 + core
        return remote(
            cols.at[slot], cols.at[slot], over_send.at[0], over_recv.at[q], (p, g, 1 - c)
        )

    over(p, c).start()
    for k in range(1, count):
        q = turn(p, k)
        at = q * 2 + c
        remote(cols.at[at], cols.at[at], col_send.at[0], col_recv.at[q], (q, g, c)).wait_recv()
        over(q, c).start()
    for slot in range(slots):
        @pl.when(slot != me)
        def _():
            remote(
                rows.at[slot], rows.at[slot], row_send.at[0], row_recv.at[slot],
                (slot // 2, g, slot % 2),
            ).wait_recv()

    for k in range(count):
        q = turn(p, k)
        over(q, 1 - c).wait_recv()

    def sent(ref, sem):
        remote(ref, ref, sem, row_recv.at[0], (p, g, 1 - c)).wait_send()

    @pl.when(g < count - 1)
    def _():
        sent(part, chain_send.at[0])

    @pl.when(g > 0)
    def _():
        sent(part, chain_send.at[1])

    sent(rows.at[pl.ds(0, slots - 1)], row_send.at[0])
    sent(cols.at[pl.ds(0, count - 1)], col_send.at[0])
    sent(cols.at[pl.ds(0, count)], over_send.at[0])


def product_kernel(prefactor, rows, cols, out, turned):
    share = out.shape[0]
    c = lax.axis_index("gcol")
    shift = rows.shape[1] - share

    @pl.when(pl.program_id(0) == 0)
    def _():
        turned[...] = rows[...].T

    left = turned[pl.ds(pl.multiple_of(c * shift, 16), share), :]
    out[...] = jnp.dot(left, cols[...], preferred_element_type=jnp.float32) * prefactor


def product(rows, cols, share, prefactor):
    depth, width = cols.shape
    span = rows.shape[1]
    tile = 640
    return pl.pallas_call(
        functools.partial(product_kernel, prefactor),
        out_shape=jax.ShapeDtypeStruct((share, width), jnp.float32),
        grid=(width // tile,),
        in_specs=[
            pl.BlockSpec((depth, span), lambda i: (0, 0)),
            pl.BlockSpec((depth, tile), lambda i: (0, i)),
        ],
        out_specs=pl.BlockSpec((share, tile), lambda i: (0, i)),
        scratch_shapes=[pltpu.VMEM((span, depth), jnp.bfloat16)],
        compiler_params=pltpu.CompilerParams(vmem_limit_bytes=24 * 1024 * 1024),
    )(rows, cols)


def fast_body(valence, conduction, val_energy, cond_energy, val_occupation, gvectors):
    nv, planes, points = valence.shape
    bands = conduction.shape[0]
    count = lax.axis_size("pair")
    gcol_count = lax.axis_size("gcol")
    height = nv * planes
    steps = QUARTER // STEP
    pairs = bands * nv
    width = 2 * KG // count
    slots = count * gcol_count
    pieces = KG // PIECE
    share = width // gcol_count
    span = width - share // 128 * 128
    bf16, f32 = jnp.bfloat16, jnp.float32
    left, right, sign = half_plane_tables()
    xtab = plane_table(nv)
    hbm = pl.BlockSpec(memory_space=pltpu.HBM)
    vmem = pl.BlockSpec(memory_space=pltpu.VMEM)
    dma = pltpu.SemaphoreType.DMA
    piece = pltpu.VMEM((pieces, 2 * pairs, PIECE), bf16)
    cols, rows = pl.pallas_call(
        chi_kernel,
        out_shape=(
            pltpu.VMEM((slots, pairs, width), bf16),
            pltpu.VMEM((slots, pairs, span), bf16),
        ),
        in_specs=[hbm] * 10,
        out_specs=(vmem, vmem),
        scratch_shapes=[
            pltpu.SMEM(val_occupation.shape, jnp.int32),
            pltpu.SMEM(val_energy.shape, f32),
            pltpu.SMEM(cond_energy.shape, f32),
            pltpu.VMEM(gvectors.shape, jnp.int32),
            pltpu.VMEM((nv + bands, planes, points), bf16),
            pltpu.VMEM(left.shape, f32),
            pltpu.VMEM(right.shape, f32),
            pltpu.VMEM(sign.shape, f32),
            pltpu.VMEM((2, planes, RAD * 4 * nv), f32),
            pltpu.VMEM((6, QUARTER, TILE), bf16),
            pltpu.VMEM((4, bands * height, QUARTER), bf16),
            pltpu.VMEM((4, bands * height, TILE), f32),
            pltpu.VMEM((2 * height, RAD * 4 * nv), bf16),
            pltpu.VMEM((RAD * NR, 128), f32),
            pltpu.VMEM((PIECE, 128), f32),
            piece, piece, piece, piece, piece, piece,
            pltpu.VMEM((1, KG), jnp.int32),
            pltpu.SMEM((1, KG), jnp.int32),
            dma((steps + 8,)),
            dma((2,)),
            dma((2, pieces // UNIT)),
            dma((1,)),
            dma((slots,)),
            dma((1,)),
            dma((count,)),
            dma((1,)),
            dma((count,)),
            dma((1,)),
        ],
        compiler_params=pltpu.CompilerParams(
            vmem_limit_bytes=60 * 1024 * 1024, collective_id=0, has_side_effects=True
        ),
    )(
        val_occupation, val_energy, cond_energy, gvectors,
        valence, conduction, left, right, sign, xtab,
    )
    all_pairs = slots * pairs
    prefactor = -1.0 / math.sqrt(all_pairs)
    return product(
        rows.reshape(all_pairs, span), cols.reshape(all_pairs, width), share, prefactor
    )


def either_body(valence, conduction, *rest):
    nv, planes, _ = valence.shape
    count = lax.axis_size("pair")
    width = 2 * KG // count
    fits = (
        count == lax.axis_size("grow")
        and count % 2 == 0
        and lax.axis_size("gcol") == 2
        and planes % 8 == 0
        and conduction.shape[0] == 2
        and 8 * nv == 128
        and width % PIECE == 0
        and width // PIECE % 2 == 1
        and KG // PIECE % UNIT == 0
    )
    return (fast_body if fits else body)(valence, conduction, *rest)


def solution(mesh):
    return jax.shard_map(
        either_body,
        mesh=mesh,
        in_specs=(P(None, "grow", None), P(("pair", "gcol"), "grow", None), P(), P(), P(), P()),
        out_specs=P(("pair", "gcol"), "grow"),
        check_vma=False,
    )
```

```python
import functools
import math

import jax
import jax.numpy as jnp
import numpy as np
from jax import lax
from jax.experimental import pallas as pl
from jax.experimental.pallas import tpu as pltpu
from jax.sharding import PartitionSpec as P

N = 96
RAD = 12
KG = 3840
NV = 16


def wave_tables(positions, frequencies):
    phases = jnp.mod(positions[:, None] * frequencies[None, :], N).astype(jnp.float32) * (
        2.0 * math.pi / N
    )
    return (jnp.cos(phases), jnp.sin(phases))


def build_tables(x_positions):
    all_freq = jnp.arange(-RAD, RAD + 1, dtype=jnp.int32)
    pos_freq = jnp.arange(1, RAD + 1, dtype=jnp.int32)
    positions = jnp.arange(N, dtype=jnp.int32)
    cosine, sine_part = wave_tables(positions, all_freq)
    z_table = jnp.concatenate([cosine, sine_part], 1).astype(jnp.bfloat16)
    y_table = jnp.stack(
        [jnp.stack([cosine, sine_part], 1), jnp.stack([-sine_part, cosine], 1)], 1
    ).astype(jnp.bfloat16)
    x_cos, x_sin = wave_tables(x_positions, pos_freq)
    x_table = jnp.stack([jnp.stack([x_cos, -x_sin], 1), jnp.stack([-x_sin, -x_cos], 1)], 1).astype(
        jnp.bfloat16
    )
    return (z_table, y_table, x_table)


def pair_product(left_rows, right_rows):
    return lax.dot_general(
        left_rows, right_rows, (((0,), (0,)), ((), ())), preferred_element_type=jnp.float32
    )


def body(valence, conduction, val_energy, cond_energy, val_occupation, gvectors):
    pair_count = lax.axis_size("pair")
    gcol_count = lax.axis_size("gcol")
    planes = valence.shape[1]
    cond_bands = conduction.shape[0]
    extent = 2 * RAD + 1
    local_pairs = cond_bands * NV
    x_positions = lax.axis_index("grow") * planes + jnp.arange(planes, dtype=jnp.int32)
    z_table, y_table, x_table = build_tables(x_positions)
    flat_index = ((gvectors[0] - 1) * extent + gvectors[1] + RAD) * extent + gvectors[2] + RAD
    density = conduction[:, None] * valence[None]
    section_one = jnp.dot(
        density.reshape(-1, N), z_table, preferred_element_type=jnp.float32
    ).astype(jnp.bfloat16)
    section_one = section_one.reshape(local_pairs * planes, N, 2, extent)
    second = jnp.einsum(
        "ayik,yioj->aojk", section_one, y_table, preferred_element_type=jnp.float32
    ).astype(jnp.bfloat16)
    second = second.reshape(local_pairs, planes, 2, extent * extent)
    section_three = jnp.einsum(
        "pxoq,xosm->psmq", second, x_table, preferred_element_type=jnp.float32
    )
    section_three = section_three.reshape(local_pairs, 2, RAD * extent * extent)
    picked = jnp.take(section_three, flat_index, axis=2).reshape(local_pairs, 2 * KG)
    summed = lax.psum_scatter(
        picked.astype(jnp.bfloat16), "grow", scatter_dimension=1, tiled=True
    ).astype(jnp.float32)
    first_band = (lax.axis_index("pair") * gcol_count + lax.axis_index("gcol")) * cond_bands
    own_energy = lax.dynamic_slice_in_dim(cond_energy, first_band, cond_bands, 0)
    weight = val_occupation.astype(jnp.float32)[None, :] / (
        4.0 * (own_energy[:, None] - val_energy[None, :])
    )
    factor = (jnp.sqrt(weight) * (1.0 / N**1.5)).reshape(local_pairs, 1)
    weighted = (summed * factor).astype(jnp.bfloat16)
    prefactor = -1.0 / math.sqrt(pair_count * gcol_count * local_pairs)
    full_rows = lax.all_gather(weighted, "grow", axis=1, tiled=True)
    row_part = lax.all_to_all(full_rows, "pair", split_axis=1, concat_axis=0, tiled=True)
    partial_value = pair_product(row_part, lax.all_gather(weighted, "pair", axis=0, tiled=True))
    return lax.psum_scatter(
        (partial_value * prefactor).astype(jnp.bfloat16), "gcol", scatter_dimension=0, tiled=True
    ).astype(jnp.float32)


EXT = 2 * RAD + 1
QUARTER = N * N // 4
STEP = 8 * N
TILE = 256
CLASSES = ((0, 4, 8, 12), (2, 6, 10), (1, 3, 5, 7, 9, 11))
WIDTHS = (128, 128, 256)
ROWS = (104, 80, 152)
STARTS = (0, 104, 184)
NR = 336
TALL = (112, 80, 160)
PIECE = 128
UNIT = 1
LAG = 6


def half_plane_tables():
    total = 2 * sum(WIDTHS)
    left = np.zeros((2, N // 4, total), np.float32)
    right = np.zeros((2, N, total), np.float32)
    sign = np.zeros((1, WIDTHS[2]), np.float32)
    y = np.arange(N // 4)[:, None]
    z = np.arange(N)[:, None]
    k = np.arange(-RAD, RAD + 1)
    base = 0
    for freqs, width in zip(CLASSES, WIDTHS):
        jj = np.repeat(np.array(freqs), EXT)[None]
        kk = np.tile(k, len(freqs))[None]
        count = jj.shape[1]
        ay = 2 * np.pi * ((jj * y) % N) / N
        az = 2 * np.pi * ((kk * z) % N) / N
        for part in range(2):
            cols = slice(base + part * width, base + part * width + count)
            left[0, :, cols] = np.sin(ay) if part else np.cos(ay)
            left[1, :, cols] = np.cos(ay) if part else -np.sin(ay)
            right[0, :, cols] = np.cos(az)
            right[1, :, cols] = np.sin(az)
        base += 2 * width
    jj = np.repeat(np.array(CLASSES[2]), EXT)
    sign[0, : jj.size] = np.where(jj % 4 == 1, 1.0, -1.0)
    return left, right, sign


def plane_table(pairs):
    x = np.arange(N)[:, None]
    a = np.arange(1, RAD + 1)[None]
    ang = 2 * np.pi * ((a * x) % N) / N
    c, s = np.cos(ang), np.sin(ang)
    tab = np.stack([np.stack([c, -s, c, -s], -1), np.stack([-s, -c, s, c], -1)])
    return np.repeat(tab.reshape(2, N, RAD * 4), pairs, axis=2).astype(np.float32)


def row_index(a, b, d):
    j = jnp.abs(b)
    k = jnp.where(b < 0, -d, d) + RAD
    row = jnp.where(
        (j & 1) == 1,
        STARTS[2] + (j >> 1) * EXT,
        jnp.where((j & 3) == 2, STARTS[1], STARTS[0]) + (j >> 2) * EXT,
    )
    return jnp.maximum((a - 1) * NR + row + k, 0)


def chi_kernel(
    occ_in, val_in, cond_in, gvec_in, val, cond, left, right, sign, xtab,
    cols, rows,
    occ, val_e, cond_e, gvec, orbitals, leftv, rightv, signv, xv, tabs, folded, acc, xmat, sec, got,
    part, rin, lin, rout, lout, tot, index, idx,
    loads, chain_send, chain_recv, row_send, row_recv, col_send, col_recv,
    over_send, over_recv, outs,
):
    f32, bf16 = jnp.float32, jnp.bfloat16
    nv, planes, _ = val.shape
    bands = cond.shape[0]
    height = nv * planes
    pairs = bands * nv
    lanes = 128
    half = lanes // 2
    steps = QUARTER // STEP
    pieces = part.shape[0]
    units = pieces // UNIT
    slots, _, width = cols.shape
    count = slots // 2
    per = width // PIECE
    middle = per // 2
    span = rows.shape[2]
    p, g, c = lax.axis_index("pair"), lax.axis_index("grow"), lax.axis_index("gcol")
    me = p * 2 + c
    turn = lambda at, k: lax.rem(at + k, count)

    def remote(src, dst, send, recv, to):
        return pltpu.make_async_remote_copy(
            src_ref=src, dst_ref=dst, send_sem=send, recv_sem=recv,
            device_id=to, device_id_type=pl.DeviceIdType.MESH,
        )

    table_loads = [
        pltpu.make_async_copy(a, b, loads.at[steps + i])
        for i, (a, b) in enumerate(
            (
                (left, leftv),
                (right, rightv),
                (sign, signv),
                (gvec_in, gvec),
                (xtab.at[:, pl.ds(pl.multiple_of(g * planes, 8), planes), :], xv),
                (occ_in, occ),
                (val_in, val_e),
                (cond_in, cond_e),
            )
        )
    ]
    step_loads = []
    for s in range(steps):
        group = []
        for q in range(4):
            at = pl.ds(q * QUARTER + s * STEP, STEP)
            for a, first in ((cond, nv), (val, 0)):
                b = orbitals.at[pl.ds(first, a.shape[0]), :, at]
                group.append(pltpu.make_async_copy(a.at[:, :, at], b, loads.at[s]))
        step_loads.append(group)
    for copy in table_loads[:4] + sum(step_loads, []) + table_loads[4:]:
        copy.start()

    barrier = pltpu.get_barrier_semaphore()
    pl.semaphore_signal(barrier, inc=1, device_id=(p, g, 1 - c))
    for k in range(1, count):
        for d in range(2):
            pl.semaphore_signal(barrier, inc=1, device_id=(turn(p, k), g, d))
        pl.semaphore_signal(barrier, inc=1, device_id=(p, turn(g, k), c))

    for copy in table_loads[:4]:
        copy.wait()
    index[...] = row_index(gvec[0:1, :], gvec[1:2, :], gvec[2:3, :])
    index_copy = pltpu.make_async_copy(index, idx, outs.at[0])
    index_copy.start()

    def table_rows(y, carry):
        l1, l2 = leftv[0, pl.ds(y, 1), :], leftv[1, pl.ds(y, 1), :]
        at = pl.ds(pl.multiple_of(y * N, 32), N)
        full = l1 * rightv[0] + l2 * rightv[1]
        odd_p, odd_q = full[:, 2 * TILE : 3 * TILE], full[:, 3 * TILE :]
        tiles = (
            full[:, 0:TILE], full[:, TILE : 2 * TILE],
            odd_p, odd_q * (0.0 - signv[...]), odd_q, odd_p * signv[...],
        )
        for i, tile in enumerate(tiles):
            tabs[i, at, :] = tile.astype(bf16)
        return carry

    lax.fori_loop(0, QUARTER // N, table_rows, 0)

    def ready(s):
        whole = orbitals.at[:, :, pl.ds(0, 4 * STEP)]
        pltpu.make_async_copy(whole, whole, loads.at[s]).wait()

    def products(i, carry):
        at = [pl.ds(pl.multiple_of(q * QUARTER + i * TILE, TILE), TILE) for q in range(4)]
        here = pl.ds(pl.multiple_of(i * TILE, TILE), TILE)
        for b in range(bands):
            for x in range(0, planes, 8):
                cs = [orbitals[nv + b, x : x + 8, q] for q in at]
                for v in range(nv):
                    d0, d1, d2, d3 = [orbitals[v, x : x + 8, q] * u for q, u in zip(at, cs)]
                    e0, e1 = d0 + d2, d1 + d3
                    row = b * height + v * planes + x
                    where = slice(row, row + 8)
                    folded[0, where, here] = e0 + e1
                    folded[1, where, here] = e0 - e1
                    folded[2, where, here] = d0 - d2
                    folded[3, where, here] = d1 - d3
        return carry

    for s in range(steps):
        ready(s)
        lax.fori_loop(s * STEP // TILE, (s + 1) * STEP // TILE, products, 0)

    dot = lambda i, j: jnp.dot(folded[i], tabs[j], preferred_element_type=f32)
    acc[0] = dot(0, 0)
    acc[1] = dot(1, 1)
    acc[2] = dot(2, 2) + dot(3, 3)
    acc[3] = dot(2, 4) + dot(3, 5)

    for copy in table_loads[4:]:
        copy.wait()
    own = lax.broadcasted_iota(jnp.int32, (1, RAD * 4 * nv), 1) % nv

    def place(v, carry):
        for h in range(2):
            two = [jnp.where(own == 2 * v + u, xv[h], 0.0) for u in range(2)]
            at = pl.multiple_of(h * height + v * 2 * planes, 16)
            xmat[pl.ds(at, 2 * planes), :] = jnp.concatenate(two, 0).astype(bf16)
        return carry

    lax.fori_loop(0, nv // 2, place, 0)

    lane = lax.broadcasted_iota(jnp.int32, (1, lanes), 1)
    occupied = jnp.zeros((1, lanes), jnp.int32)
    energy = jnp.zeros((1, lanes), f32)
    for v in range(nv):
        occupied = jnp.where(lane % nv == v, occ[v], occupied)
        energy = jnp.where(lane % nv == v, val_e[v], energy)
    factors = [
        jnp.sqrt(occupied.astype(f32) / (4.0 * (cond_e[me * bands + b] - energy)))
        * (1.0 / N**1.5)
        for b in range(bands)
    ]
    lower = lane < half
    groups = (
        ((0,), (0,), (0, 128), 128, TALL[0], ROWS[0], STARTS[0]),
        ((1,), (1,), (0, 128), 128, TALL[1], ROWS[1], STARTS[1]),
        ((2,), (3,), (0, 0), 256, TALL[2], ROWS[2], STARTS[2]),
    )
    for first_of, second_of, bases, size_of, tall, size, start in groups:
        summed = []
        for b in range(bands):
            at = slice(b * height, (b + 1) * height)
            turned = [
                sum(acc[i, at, base : base + size_of] for i in which).astype(bf16).T[0:tall]
                for which, base in zip((first_of, second_of), bases)
            ]
            summed.append(
                jnp.dot(jnp.concatenate(turned, 1), xmat[...], preferred_element_type=f32)
            )
        for t in range(RAD // 2):
            first, second = [
                summed[b][0:size, t * lanes : (t + 1) * lanes] * factors[b] for b in range(bands)
            ]
            second = pltpu.roll(second, half, 1)
            at = 2 * t * NR + start
            sec[at : at + size, :] = jnp.where(lower, first, second)
            sec[at + NR : at + NR + size, :] = jnp.where(lower, second, first)

    index_copy.wait()
    pl.semaphore_wait(barrier, 1 + 3 * (count - 1))

    def pick(n):
        at = pl.ds(pl.multiple_of(n * PIECE, PIECE), PIECE)
        for u in range(PIECE):
            got[u : u + 1, :] = sec[pl.ds(idx[0, n * PIECE + u], 1), :]
        turned = got[...].T
        odd = ((gvec[0:1, at] - 1) & 1) == 1
        flip = gvec[1:2, at] < 0
        top, bottom = turned[0:half], turned[half:lanes]
        for b, both in enumerate((jnp.where(odd, bottom, top), jnp.where(odd, top, bottom))):
            chosen = jnp.where(flip, both[2 * nv : 4 * nv], both[0 : 2 * nv]).astype(bf16)
            part[n, b * nv : (b + 1) * nv, :] = chosen[0:nv]
            part[n, pairs + b * nv : pairs + (b + 1) * nv, :] = chosen[nv : 2 * nv]

    def right_copy(src, t):
        at = pl.ds(t * UNIT, UNIT)
        return remote(
            src.at[at], rin.at[at], chain_send.at[0], chain_recv.at[0, t],
            (p, jnp.minimum(g + 1, count - 1), c),
        )

    def left_copy(src, t):
        at = pl.ds(t * UNIT, UNIT)
        return remote(
            src.at[at], lin.at[at], chain_send.at[1], chain_recv.at[1, t],
            (p, jnp.maximum(g - 1, 0), c),
        )

    def chain(t, make, came, passed, first, last):
        @pl.when((t >= 0) & (t < units))
        def _():
            @pl.when(first)
            def _():
                make(part, t).start()

            @pl.when(jnp.logical_not(first))
            def _():
                make(part, t).wait_recv()

                @pl.when(jnp.logical_not(last))
                def _():
                    at = pl.ds(t * UNIT, UNIT)
                    passed[at] = (part[at].astype(f32) + came[at].astype(f32)).astype(bf16)
                    make(passed, t).start()

    def row_copy(t, r, b, d, j):
        at = pl.ds(pl.multiple_of(j * PIECE, PIECE), PIECE)
        return remote(
            tot.at[t, pl.ds(r * pairs, pairs), :], rows.at[me, :, at],
            row_send.at[0], row_recv.at[me], (b, g, d),
        )

    def put(t, r, b, d, j):
        here = (b == p) & (d == c)

        @pl.when(here)
        def _():
            at = pl.ds(pl.multiple_of(j * PIECE, PIECE), PIECE)
            rows[me, :, at] = tot[t, r * pairs : (r + 1) * pairs, :]

        @pl.when(jnp.logical_not(here))
        def _():
            row_copy(t, r, b, d, j).start()

    def col_copy(t, r, j, k):
        at = pl.ds(pl.multiple_of(j * PIECE, 128), PIECE)
        return remote(
            tot.at[t, pl.ds(r * pairs, pairs), :], cols.at[me, :, at],
            col_send.at[0], col_recv.at[p], (turn(p, k), g, c),
        )

    def deliver(t):
        h = t // per
        j = t - h * per
        for r in range(2):
            b = h + r * (count // 2)

            @pl.when(j <= middle)
            def _():
                put(t, r, b, 0, j)

            @pl.when(j >= middle)
            def _():
                put(t, r, b, 1, j - middle)

            @pl.when(b == g)
            def _():
                at = pl.ds(pl.multiple_of(j * PIECE, 128), PIECE)
                cols[me, :, at] = tot[t, r * pairs : (r + 1) * pairs, :]
                for k in range(1, count):
                    col_copy(t, r, j, k).start()

    def finish(u):
        @pl.when((u >= 0) & (u < units))
        def _():
            at = pl.ds(u * UNIT, UNIT)
            mine = lambda: part[at].astype(f32)

            @pl.when(g == 0)
            def _():
                tot[at] = (mine() + lin[at].astype(f32)).astype(bf16)

            @pl.when(g == count - 1)
            def _():
                tot[at] = (mine() + rin[at].astype(f32)).astype(bf16)

            @pl.when((g > 0) & (g < count - 1))
            def _():
                tot[at] = (mine() + rin[at].astype(f32) + lin[at].astype(f32)).astype(bf16)

            for i in range(UNIT):
                deliver(u * UNIT + i)

    def serve(n):
        to_right = n - g * LAG
        to_left = n - (count - 1 - g) * LAG
        chain(to_right, right_copy, rin, rout, g == 0, g == count - 1)
        chain(to_left, left_copy, lin, lout, g == count - 1, g == 0)
        finish(jnp.minimum(to_right, to_left))

    def early(n, carry):
        for i in range(UNIT):
            pick(n * UNIT + i)
        serve(n)
        return carry

    def late(n, carry):
        serve(n)
        return carry

    lax.fori_loop(0, units, early, 0)
    lax.fori_loop(units, units + LAG * (count - 1), late, 0)

    def over(q, core):
        slot = q * 2 + core
        return remote(
            cols.at[slot], cols.at[slot], over_send.at[0], over_recv.at[q], (p, g, 1 - c)
        )

    over(p, c).start()
    for k in range(1, count):
        q = turn(p, k)
        at = q * 2 + c
        remote(cols.at[at], cols.at[at], col_send.at[0], col_recv.at[q], (q, g, c)).wait_recv()
        over(q, c).start()
    for slot in range(slots):
        @pl.when(slot != me)
        def _():
            remote(
                rows.at[slot], rows.at[slot], row_send.at[0], row_recv.at[slot],
                (slot // 2, g, slot % 2),
            ).wait_recv()

    for k in range(count):
        q = turn(p, k)
        over(q, 1 - c).wait_recv()

    def sent(ref, sem):
        remote(ref, ref, sem, row_recv.at[0], (p, g, 1 - c)).wait_send()

    @pl.when(g < count - 1)
    def _():
        sent(part, chain_send.at[0])

    @pl.when(g > 0)
    def _():
        sent(part, chain_send.at[1])

    sent(rows.at[pl.ds(0, slots - 1)], row_send.at[0])
    sent(cols.at[pl.ds(0, count - 1)], col_send.at[0])
    sent(cols.at[pl.ds(0, count)], over_send.at[0])


def product_kernel(prefactor, tile, rows, cols, out, turned, held, sems):
    share, width = out.shape
    c = lax.axis_index("gcol")
    shift = rows.shape[1] - share
    turned[...] = rows[...].T
    left = turned[pl.ds(pl.multiple_of(c * shift, 16), share), :]
    copies = []
    for i, start in enumerate(range(0, width, tile)):
        at = pl.ds(start, min(tile, width - start))
        held[:, at] = jnp.dot(left, cols[:, at], preferred_element_type=jnp.float32) * prefactor
        copies.append(pltpu.make_async_copy(held.at[:, at], out.at[:, at], sems.at[i]))
        copies[-1].start()
    for copy in copies:
        copy.wait()


def product(rows, cols, share, prefactor):
    depth, width = cols.shape
    span = rows.shape[1]
    tile = 512
    vmem = pl.BlockSpec(memory_space=pltpu.VMEM)
    return pl.pallas_call(
        functools.partial(product_kernel, prefactor, tile),
        out_shape=jax.ShapeDtypeStruct((share, width), jnp.float32),
        in_specs=[vmem, vmem],
        out_specs=pl.BlockSpec(memory_space=pltpu.HBM),
        scratch_shapes=[
            pltpu.VMEM((span, depth), jnp.bfloat16),
            pltpu.VMEM((share, width), jnp.float32),
            pltpu.SemaphoreType.DMA((pl.cdiv(width, tile),)),
        ],
        compiler_params=pltpu.CompilerParams(vmem_limit_bytes=24 * 1024 * 1024),
    )(rows, cols)


def fast_body(valence, conduction, val_energy, cond_energy, val_occupation, gvectors):
    nv, planes, points = valence.shape
    bands = conduction.shape[0]
    count = lax.axis_size("pair")
    gcol_count = lax.axis_size("gcol")
    height = nv * planes
    steps = QUARTER // STEP
    pairs = bands * nv
    width = 2 * KG // count
    slots = count * gcol_count
    pieces = KG // PIECE
    share = width // gcol_count
    span = width - share // 128 * 128
    bf16, f32 = jnp.bfloat16, jnp.float32
    left, right, sign = half_plane_tables()
    xtab = plane_table(nv)
    hbm = pl.BlockSpec(memory_space=pltpu.HBM)
    vmem = pl.BlockSpec(memory_space=pltpu.VMEM)
    dma = pltpu.SemaphoreType.DMA
    piece = pltpu.VMEM((pieces, 2 * pairs, PIECE), bf16)
    cols, rows = pl.pallas_call(
        chi_kernel,
        out_shape=(
            pltpu.VMEM((slots, pairs, width), bf16),
            pltpu.VMEM((slots, pairs, span), bf16),
        ),
        in_specs=[hbm] * 10,
        out_specs=(vmem, vmem),
        scratch_shapes=[
            pltpu.SMEM(val_occupation.shape, jnp.int32),
            pltpu.SMEM(val_energy.shape, f32),
            pltpu.SMEM(cond_energy.shape, f32),
            pltpu.VMEM(gvectors.shape, jnp.int32),
            pltpu.VMEM((nv + bands, planes, points), bf16),
            pltpu.VMEM(left.shape, f32),
            pltpu.VMEM(right.shape, f32),
            pltpu.VMEM(sign.shape, f32),
            pltpu.VMEM((2, planes, RAD * 4 * nv), f32),
            pltpu.VMEM((6, QUARTER, TILE), bf16),
            pltpu.VMEM((4, bands * height, QUARTER), bf16),
            pltpu.VMEM((4, bands * height, TILE), f32),
            pltpu.VMEM((2 * height, RAD * 4 * nv), bf16),
            pltpu.VMEM((RAD * NR, 128), f32),
            pltpu.VMEM((PIECE, 128), f32),
            piece, piece, piece, piece, piece, piece,
            pltpu.VMEM((1, KG), jnp.int32),
            pltpu.SMEM((1, KG), jnp.int32),
            dma((steps + 8,)),
            dma((2,)),
            dma((2, pieces // UNIT)),
            dma((1,)),
            dma((slots,)),
            dma((1,)),
            dma((count,)),
            dma((1,)),
            dma((count,)),
            dma((1,)),
        ],
        compiler_params=pltpu.CompilerParams(
            vmem_limit_bytes=60 * 1024 * 1024, collective_id=0, has_side_effects=True
        ),
    )(
        val_occupation, val_energy, cond_energy, gvectors,
        valence, conduction, left, right, sign, xtab,
    )
    all_pairs = slots * pairs
    prefactor = -1.0 / math.sqrt(all_pairs)
    return product(
        rows.reshape(all_pairs, span), cols.reshape(all_pairs, width), share, prefactor
    )


def either_body(valence, conduction, *rest):
    nv, planes, _ = valence.shape
    count = lax.axis_size("pair")
    width = 2 * KG // count
    fits = (
        count == lax.axis_size("grow")
        and count % 2 == 0
        and lax.axis_size("gcol") == 2
        and planes % 8 == 0
        and conduction.shape[0] == 2
        and 8 * nv == 128
        and width % PIECE == 0
        and width // PIECE % 2 == 1
        and KG // PIECE % UNIT == 0
    )
    return (fast_body if fits else body)(valence, conduction, *rest)


def solution(mesh):
    return jax.shard_map(
        either_body,
        mesh=mesh,
        in_specs=(P(None, "grow", None), P(("pair", "gcol"), "grow", None), P(), P(), P(), P()),
        out_specs=P(("pair", "gcol"), "grow"),
        check_vma=False,
    )
```

```python
import functools
import math

import jax
import jax.numpy as jnp
import numpy as np
from jax import lax
from jax.experimental import pallas as pl
from jax.experimental.pallas import tpu as pltpu
from jax.sharding import PartitionSpec as P

N = 96
RAD = 12
KG = 3840
NV = 16


def wave_tables(positions, frequencies):
    phases = jnp.mod(positions[:, None] * frequencies[None, :], N).astype(jnp.float32) * (
        2.0 * math.pi / N
    )
    return (jnp.cos(phases), jnp.sin(phases))


def build_tables(x_positions):
    all_freq = jnp.arange(-RAD, RAD + 1, dtype=jnp.int32)
    pos_freq = jnp.arange(1, RAD + 1, dtype=jnp.int32)
    positions = jnp.arange(N, dtype=jnp.int32)
    cosine, sine_part = wave_tables(positions, all_freq)
    z_table = jnp.concatenate([cosine, sine_part], 1).astype(jnp.bfloat16)
    y_table = jnp.stack(
        [jnp.stack([cosine, sine_part], 1), jnp.stack([-sine_part, cosine], 1)], 1
    ).astype(jnp.bfloat16)
    x_cos, x_sin = wave_tables(x_positions, pos_freq)
    x_table = jnp.stack([jnp.stack([x_cos, -x_sin], 1), jnp.stack([-x_sin, -x_cos], 1)], 1).astype(
        jnp.bfloat16
    )
    return (z_table, y_table, x_table)


def pair_product(left_rows, right_rows):
    return lax.dot_general(
        left_rows, right_rows, (((0,), (0,)), ((), ())), preferred_element_type=jnp.float32
    )


def body(valence, conduction, val_energy, cond_energy, val_occupation, gvectors):
    pair_count = lax.axis_size("pair")
    gcol_count = lax.axis_size("gcol")
    planes = valence.shape[1]
    cond_bands = conduction.shape[0]
    extent = 2 * RAD + 1
    local_pairs = cond_bands * NV
    x_positions = lax.axis_index("grow") * planes + jnp.arange(planes, dtype=jnp.int32)
    z_table, y_table, x_table = build_tables(x_positions)
    flat_index = ((gvectors[0] - 1) * extent + gvectors[1] + RAD) * extent + gvectors[2] + RAD
    density = conduction[:, None] * valence[None]
    section_one = jnp.dot(
        density.reshape(-1, N), z_table, preferred_element_type=jnp.float32
    ).astype(jnp.bfloat16)
    section_one = section_one.reshape(local_pairs * planes, N, 2, extent)
    second = jnp.einsum(
        "ayik,yioj->aojk", section_one, y_table, preferred_element_type=jnp.float32
    ).astype(jnp.bfloat16)
    second = second.reshape(local_pairs, planes, 2, extent * extent)
    section_three = jnp.einsum(
        "pxoq,xosm->psmq", second, x_table, preferred_element_type=jnp.float32
    )
    section_three = section_three.reshape(local_pairs, 2, RAD * extent * extent)
    picked = jnp.take(section_three, flat_index, axis=2).reshape(local_pairs, 2 * KG)
    summed = lax.psum_scatter(
        picked.astype(jnp.bfloat16), "grow", scatter_dimension=1, tiled=True
    ).astype(jnp.float32)
    first_band = (lax.axis_index("pair") * gcol_count + lax.axis_index("gcol")) * cond_bands
    own_energy = lax.dynamic_slice_in_dim(cond_energy, first_band, cond_bands, 0)
    weight = val_occupation.astype(jnp.float32)[None, :] / (
        4.0 * (own_energy[:, None] - val_energy[None, :])
    )
    factor = (jnp.sqrt(weight) * (1.0 / N**1.5)).reshape(local_pairs, 1)
    weighted = (summed * factor).astype(jnp.bfloat16)
    prefactor = -1.0 / math.sqrt(pair_count * gcol_count * local_pairs)
    full_rows = lax.all_gather(weighted, "grow", axis=1, tiled=True)
    row_part = lax.all_to_all(full_rows, "pair", split_axis=1, concat_axis=0, tiled=True)
    partial_value = pair_product(row_part, lax.all_gather(weighted, "pair", axis=0, tiled=True))
    return lax.psum_scatter(
        (partial_value * prefactor).astype(jnp.bfloat16), "gcol", scatter_dimension=0, tiled=True
    ).astype(jnp.float32)


EXT = 2 * RAD + 1
QUARTER = N * N // 4
STEP = 8 * N
TILE = 256
CLASSES = ((0, 4, 8, 12), (2, 6, 10), (1, 3, 5, 7, 9, 11))
WIDTHS = (128, 128, 256)
ROWS = (104, 80, 152)
STARTS = (0, 104, 184)
NR = 336
TALL = (112, 80, 160)
PIECE = 128
UNIT = 1
LAG = 6


def half_plane_tables():
    total = 2 * sum(WIDTHS)
    left = np.zeros((2, N // 4, total), np.float32)
    right = np.zeros((2, N, total), np.float32)
    sign = np.zeros((1, WIDTHS[2]), np.float32)
    y = np.arange(N // 4)[:, None]
    z = np.arange(N)[:, None]
    k = np.arange(-RAD, RAD + 1)
    base = 0
    for freqs, width in zip(CLASSES, WIDTHS):
        jj = np.repeat(np.array(freqs), EXT)[None]
        kk = np.tile(k, len(freqs))[None]
        count = jj.shape[1]
        ay = 2 * np.pi * ((jj * y) % N) / N
        az = 2 * np.pi * ((kk * z) % N) / N
        for part in range(2):
            cols = slice(base + part * width, base + part * width + count)
            left[0, :, cols] = np.sin(ay) if part else np.cos(ay)
            left[1, :, cols] = np.cos(ay) if part else -np.sin(ay)
            right[0, :, cols] = np.cos(az)
            right[1, :, cols] = np.sin(az)
        base += 2 * width
    jj = np.repeat(np.array(CLASSES[2]), EXT)
    sign[0, : jj.size] = np.where(jj % 4 == 1, 1.0, -1.0)
    return left, right, sign


def plane_table(pairs):
    x = np.arange(N)[:, None]
    a = np.arange(1, RAD + 1)[None]
    ang = 2 * np.pi * ((a * x) % N) / N
    c, s = np.cos(ang), np.sin(ang)
    tab = np.stack([np.stack([c, -s, c, -s], -1), np.stack([-s, -c, s, c], -1)])
    return np.repeat(tab.reshape(2, N, RAD * 4), pairs, axis=2).astype(np.float32)


def row_index(a, b, d):
    j = jnp.abs(b)
    k = jnp.where(b < 0, -d, d) + RAD
    row = jnp.where(
        (j & 1) == 1,
        STARTS[2] + (j >> 1) * EXT,
        jnp.where((j & 3) == 2, STARTS[1], STARTS[0]) + (j >> 2) * EXT,
    )
    return jnp.maximum((a - 1) * NR + row + k, 0)


def chi_kernel(
    occ_in, val_in, cond_in, gvec_in, val, cond, left, right, sign, xtab,
    cols, rows,
    occ, val_e, cond_e, gvec, orbitals, leftv, rightv, signv, xv, tabs, folded, acc, xmat, sec, got,
    part, rin, lin, rout, lout, tot, index, idx,
    loads, chain_send, chain_recv, row_send, row_recv, col_send, col_recv,
    over_send, over_recv, outs,
):
    f32, bf16 = jnp.float32, jnp.bfloat16
    nv, planes, _ = val.shape
    bands = cond.shape[0]
    height = nv * planes
    pairs = bands * nv
    lanes = 128
    half = lanes // 2
    steps = QUARTER // STEP
    pieces = part.shape[0]
    units = pieces // UNIT
    slots, _, width = cols.shape
    count = slots // 2
    per = width // PIECE
    middle = per // 2
    span = rows.shape[2]
    p, g, c = lax.axis_index("pair"), lax.axis_index("grow"), lax.axis_index("gcol")
    me = p * 2 + c
    turn = lambda at, k: lax.rem(at + k, count)

    def remote(src, dst, send, recv, to):
        return pltpu.make_async_remote_copy(
            src_ref=src, dst_ref=dst, send_sem=send, recv_sem=recv,
            device_id=to, device_id_type=pl.DeviceIdType.MESH,
        )

    table_loads = [
        pltpu.make_async_copy(a, b, loads.at[steps + i])
        for i, (a, b) in enumerate(
            (
                (left, leftv),
                (right, rightv),
                (sign, signv),
                (gvec_in, gvec),
                (xtab.at[:, pl.ds(pl.multiple_of(g * planes, 8), planes), :], xv),
                (occ_in, occ),
                (val_in, val_e),
                (cond_in, cond_e),
            )
        )
    ]
    step_loads = []
    for s in range(steps):
        group = []
        for q in range(4):
            at = pl.ds(q * QUARTER + s * STEP, STEP)
            for a, first in ((cond, nv), (val, 0)):
                b = orbitals.at[pl.ds(first, a.shape[0]), :, at]
                group.append(pltpu.make_async_copy(a.at[:, :, at], b, loads.at[s]))
        step_loads.append(group)
    for copy in table_loads[:4] + sum(step_loads, []) + table_loads[4:]:
        copy.start()

    barrier = pltpu.get_barrier_semaphore()
    pl.semaphore_signal(barrier, inc=1, device_id=(p, g, 1 - c))
    for k in range(1, count):
        for d in range(2):
            pl.semaphore_signal(barrier, inc=1, device_id=(turn(p, k), g, d))
        pl.semaphore_signal(barrier, inc=1, device_id=(p, turn(g, k), c))

    for copy in table_loads[:4]:
        copy.wait()
    index[...] = row_index(gvec[0:1, :], gvec[1:2, :], gvec[2:3, :])
    index_copy = pltpu.make_async_copy(index, idx, outs.at[0])
    index_copy.start()

    def table_rows(y, carry):
        l1, l2 = leftv[0, pl.ds(y, 1), :], leftv[1, pl.ds(y, 1), :]
        at = pl.ds(pl.multiple_of(y * N, 32), N)
        full = l1 * rightv[0] + l2 * rightv[1]
        odd_p, odd_q = full[:, 2 * TILE : 3 * TILE], full[:, 3 * TILE :]
        tiles = (
            full[:, 0:TILE], full[:, TILE : 2 * TILE],
            odd_p, odd_q * (0.0 - signv[...]), odd_q, odd_p * signv[...],
        )
        for i, tile in enumerate(tiles):
            tabs[i, at, :] = tile.astype(bf16)
        return carry

    lax.fori_loop(0, QUARTER // N, table_rows, 0)

    def ready(s):
        whole = orbitals.at[:, :, pl.ds(0, 4 * STEP)]
        pltpu.make_async_copy(whole, whole, loads.at[s]).wait()

    def products(i, carry):
        at = [pl.ds(pl.multiple_of(q * QUARTER + i * TILE, TILE), TILE) for q in range(4)]
        here = pl.ds(pl.multiple_of(i * TILE, TILE), TILE)
        for b in range(bands):
            for x in range(0, planes, 8):
                cs = [orbitals[nv + b, x : x + 8, q] for q in at]
                for v in range(nv):
                    d0, d1, d2, d3 = [orbitals[v, x : x + 8, q] * u for q, u in zip(at, cs)]
                    e0, e1 = d0 + d2, d1 + d3
                    row = b * height + v * planes + x
                    where = slice(row, row + 8)
                    folded[0, where, here] = e0 + e1
                    folded[1, where, here] = e0 - e1
                    folded[2, where, here] = d0 - d2
                    folded[3, where, here] = d1 - d3
        return carry

    for s in range(steps):
        ready(s)
        lax.fori_loop(s * STEP // TILE, (s + 1) * STEP // TILE, products, 0)

    dot = lambda i, j: jnp.dot(folded[i], tabs[j], preferred_element_type=f32)
    acc[0] = dot(0, 0).astype(bf16)
    acc[1] = dot(1, 1).astype(bf16)
    acc[2] = (dot(2, 2) + dot(3, 3)).astype(bf16)
    acc[3] = (dot(2, 4) + dot(3, 5)).astype(bf16)

    for copy in table_loads[4:]:
        copy.wait()
    own = lax.broadcasted_iota(jnp.int32, (1, RAD * 4 * nv), 1) % nv

    def place(v, carry):
        for h in range(2):
            two = [jnp.where(own == 2 * v + u, xv[h], 0.0) for u in range(2)]
            at = pl.multiple_of(h * height + v * 2 * planes, 16)
            xmat[pl.ds(at, 2 * planes), :] = jnp.concatenate(two, 0).astype(bf16)
        return carry

    lax.fori_loop(0, nv // 2, place, 0)

    lane = lax.broadcasted_iota(jnp.int32, (1, lanes), 1)
    occupied = jnp.zeros((1, lanes), jnp.int32)
    energy = jnp.zeros((1, lanes), f32)
    for v in range(nv):
        occupied = jnp.where(lane % nv == v, occ[v], occupied)
        energy = jnp.where(lane % nv == v, val_e[v], energy)
    factors = [
        jnp.sqrt(occupied.astype(f32) / (4.0 * (cond_e[me * bands + b] - energy)))
        * (1.0 / N**1.5)
        for b in range(bands)
    ]
    lower = lane < half
    groups = (
        (0, 0, (0, 128), 128, TALL[0], ROWS[0], STARTS[0]),
        (1, 1, (0, 128), 128, TALL[1], ROWS[1], STARTS[1]),
        (2, 3, (0, 0), 256, TALL[2], ROWS[2], STARTS[2]),
    )
    for first_of, second_of, bases, size_of, tall, size, start in groups:
        summed = []
        for b in range(bands):
            at = slice(b * height, (b + 1) * height)
            turned = [
                acc[which, at, base : base + size_of].T[0:tall]
                for which, base in zip((first_of, second_of), bases)
            ]
            summed.append(
                jnp.dot(jnp.concatenate(turned, 1), xmat[...], preferred_element_type=f32)
            )
        for t in range(RAD // 2):
            first, second = [
                summed[b][0:size, t * lanes : (t + 1) * lanes] * factors[b] for b in range(bands)
            ]
            second = pltpu.roll(second, half, 1)
            at = 2 * t * NR + start
            sec[at : at + size, :] = jnp.where(lower, first, second)
            sec[at + NR : at + NR + size, :] = jnp.where(lower, second, first)

    index_copy.wait()
    pl.semaphore_wait(barrier, 1 + 3 * (count - 1))

    def pick(n):
        at = pl.ds(pl.multiple_of(n * PIECE, PIECE), PIECE)
        for u in range(PIECE):
            got[u : u + 1, :] = sec[pl.ds(idx[0, n * PIECE + u], 1), :]
        turned = got[...].T
        odd = ((gvec[0:1, at] - 1) & 1) == 1
        flip = gvec[1:2, at] < 0
        top, bottom = turned[0:half], turned[half:lanes]
        for b, both in enumerate((jnp.where(odd, bottom, top), jnp.where(odd, top, bottom))):
            chosen = jnp.where(flip, both[2 * nv : 4 * nv], both[0 : 2 * nv]).astype(bf16)
            part[n, b * nv : (b + 1) * nv, :] = chosen[0:nv]
            part[n, pairs + b * nv : pairs + (b + 1) * nv, :] = chosen[nv : 2 * nv]

    def right_copy(src, t):
        at = pl.ds(t * UNIT, UNIT)
        return remote(
            src.at[at], rin.at[at], chain_send.at[0], chain_recv.at[0, t],
            (p, jnp.minimum(g + 1, count - 1), c),
        )

    def left_copy(src, t):
        at = pl.ds(t * UNIT, UNIT)
        return remote(
            src.at[at], lin.at[at], chain_send.at[1], chain_recv.at[1, t],
            (p, jnp.maximum(g - 1, 0), c),
        )

    def chain(t, make, came, passed, first, last):
        @pl.when((t >= 0) & (t < units))
        def _():
            @pl.when(first)
            def _():
                make(part, t).start()

            @pl.when(jnp.logical_not(first))
            def _():
                make(part, t).wait_recv()

                @pl.when(jnp.logical_not(last))
                def _():
                    at = pl.ds(t * UNIT, UNIT)
                    passed[at] = (part[at].astype(f32) + came[at].astype(f32)).astype(bf16)
                    make(passed, t).start()

    def row_copy(t, r, b, d, j):
        at = pl.ds(pl.multiple_of(j * PIECE, PIECE), PIECE)
        return remote(
            tot.at[t, pl.ds(r * pairs, pairs), :], rows.at[me, :, at],
            row_send.at[0], row_recv.at[me], (b, g, d),
        )

    def put(t, r, b, d, j):
        here = (b == p) & (d == c)

        @pl.when(here)
        def _():
            at = pl.ds(pl.multiple_of(j * PIECE, PIECE), PIECE)
            rows[me, :, at] = tot[t, r * pairs : (r + 1) * pairs, :]

        @pl.when(jnp.logical_not(here))
        def _():
            row_copy(t, r, b, d, j).start()

    def col_copy(t, r, j, k):
        at = pl.ds(pl.multiple_of(j * PIECE, 128), PIECE)
        return remote(
            tot.at[t, pl.ds(r * pairs, pairs), :], cols.at[me, :, at],
            col_send.at[0], col_recv.at[p], (turn(p, k), g, c),
        )

    def deliver(t):
        h = t // per
        j = t - h * per
        for r in range(2):
            b = h + r * (count // 2)

            @pl.when(j <= middle)
            def _():
                put(t, r, b, 0, j)

            @pl.when(j >= middle)
            def _():
                put(t, r, b, 1, j - middle)

            @pl.when(b == g)
            def _():
                at = pl.ds(pl.multiple_of(j * PIECE, 128), PIECE)
                cols[me, :, at] = tot[t, r * pairs : (r + 1) * pairs, :]
                for k in range(1, count):
                    col_copy(t, r, j, k).start()

    def finish(u):
        @pl.when((u >= 0) & (u < units))
        def _():
            at = pl.ds(u * UNIT, UNIT)
            mine = lambda: part[at].astype(f32)

            @pl.when(g == 0)
            def _():
                tot[at] = (mine() + lin[at].astype(f32)).astype(bf16)

            @pl.when(g == count - 1)
            def _():
                tot[at] = (mine() + rin[at].astype(f32)).astype(bf16)

            @pl.when((g > 0) & (g < count - 1))
            def _():
                tot[at] = (mine() + rin[at].astype(f32) + lin[at].astype(f32)).astype(bf16)

            for i in range(UNIT):
                deliver(u * UNIT + i)

    def serve(n):
        to_right = n - g * LAG
        to_left = n - (count - 1 - g) * LAG
        chain(to_right, right_copy, rin, rout, g == 0, g == count - 1)
        chain(to_left, left_copy, lin, lout, g == count - 1, g == 0)
        finish(jnp.minimum(to_right, to_left))

    def early(n, carry):
        for i in range(UNIT):
            pick(n * UNIT + i)
        serve(n)
        return carry

    def late(n, carry):
        serve(n)
        return carry

    lax.fori_loop(0, units, early, 0)
    lax.fori_loop(units, units + LAG * (count - 1), late, 0)

    def over(q, core):
        slot = q * 2 + core
        return remote(
            cols.at[slot], cols.at[slot], over_send.at[0], over_recv.at[q], (p, g, 1 - c)
        )

    over(p, c).start()
    for k in range(1, count):
        q = turn(p, k)
        at = q * 2 + c
        remote(cols.at[at], cols.at[at], col_send.at[0], col_recv.at[q], (q, g, c)).wait_recv()
        over(q, c).start()
    for slot in range(slots):
        @pl.when(slot != me)
        def _():
            remote(
                rows.at[slot], rows.at[slot], row_send.at[0], row_recv.at[slot],
                (slot // 2, g, slot % 2),
            ).wait_recv()

    for k in range(count):
        q = turn(p, k)
        over(q, 1 - c).wait_recv()

    def sent(ref, sem):
        remote(ref, ref, sem, row_recv.at[0], (p, g, 1 - c)).wait_send()

    @pl.when(g < count - 1)
    def _():
        sent(part, chain_send.at[0])

    @pl.when(g > 0)
    def _():
        sent(part, chain_send.at[1])

    sent(rows.at[pl.ds(0, slots - 1)], row_send.at[0])
    sent(cols.at[pl.ds(0, count - 1)], col_send.at[0])
    sent(cols.at[pl.ds(0, count)], over_send.at[0])


def product_kernel(prefactor, tile, rows, cols, out, turned, held, sems):
    share, width = out.shape
    c = lax.axis_index("gcol")
    shift = rows.shape[1] - share
    turned[...] = rows[...].T
    left = turned[pl.ds(pl.multiple_of(c * shift, 16), share), :]
    copies = []
    for i, start in enumerate(range(0, width, tile)):
        at = pl.ds(start, min(tile, width - start))
        held[:, at] = jnp.dot(left, cols[:, at], preferred_element_type=jnp.float32) * prefactor
        copies.append(pltpu.make_async_copy(held.at[:, at], out.at[:, at], sems.at[i]))
        copies[-1].start()
    for copy in copies:
        copy.wait()


def product(rows, cols, share, prefactor):
    depth, width = cols.shape
    span = rows.shape[1]
    tile = 512
    vmem = pl.BlockSpec(memory_space=pltpu.VMEM)
    return pl.pallas_call(
        functools.partial(product_kernel, prefactor, tile),
        out_shape=jax.ShapeDtypeStruct((share, width), jnp.float32),
        in_specs=[vmem, vmem],
        out_specs=pl.BlockSpec(memory_space=pltpu.HBM),
        scratch_shapes=[
            pltpu.VMEM((span, depth), jnp.bfloat16),
            pltpu.VMEM((share, width), jnp.float32),
            pltpu.SemaphoreType.DMA((pl.cdiv(width, tile),)),
        ],
        compiler_params=pltpu.CompilerParams(vmem_limit_bytes=24 * 1024 * 1024),
    )(rows, cols)


def fast_body(valence, conduction, val_energy, cond_energy, val_occupation, gvectors):
    nv, planes, points = valence.shape
    bands = conduction.shape[0]
    count = lax.axis_size("pair")
    gcol_count = lax.axis_size("gcol")
    height = nv * planes
    steps = QUARTER // STEP
    pairs = bands * nv
    width = 2 * KG // count
    slots = count * gcol_count
    pieces = KG // PIECE
    share = width // gcol_count
    span = width - share // 128 * 128
    bf16, f32 = jnp.bfloat16, jnp.float32
    left, right, sign = half_plane_tables()
    xtab = plane_table(nv)
    hbm = pl.BlockSpec(memory_space=pltpu.HBM)
    vmem = pl.BlockSpec(memory_space=pltpu.VMEM)
    dma = pltpu.SemaphoreType.DMA
    piece = pltpu.VMEM((pieces, 2 * pairs, PIECE), bf16)
    cols, rows = pl.pallas_call(
        chi_kernel,
        out_shape=(
            pltpu.VMEM((slots, pairs, width), bf16),
            pltpu.VMEM((slots, pairs, span), bf16),
        ),
        in_specs=[hbm] * 10,
        out_specs=(vmem, vmem),
        scratch_shapes=[
            pltpu.SMEM(val_occupation.shape, jnp.int32),
            pltpu.SMEM(val_energy.shape, f32),
            pltpu.SMEM(cond_energy.shape, f32),
            pltpu.VMEM(gvectors.shape, jnp.int32),
            pltpu.VMEM((nv + bands, planes, points), bf16),
            pltpu.VMEM(left.shape, f32),
            pltpu.VMEM(right.shape, f32),
            pltpu.VMEM(sign.shape, f32),
            pltpu.VMEM((2, planes, RAD * 4 * nv), f32),
            pltpu.VMEM((6, QUARTER, TILE), bf16),
            pltpu.VMEM((4, bands * height, QUARTER), bf16),
            pltpu.VMEM((4, bands * height, TILE), bf16),
            pltpu.VMEM((2 * height, RAD * 4 * nv), bf16),
            pltpu.VMEM((RAD * NR, 128), f32),
            pltpu.VMEM((PIECE, 128), f32),
            piece, piece, piece, piece, piece, piece,
            pltpu.VMEM((1, KG), jnp.int32),
            pltpu.SMEM((1, KG), jnp.int32),
            dma((steps + 8,)),
            dma((2,)),
            dma((2, pieces // UNIT)),
            dma((1,)),
            dma((slots,)),
            dma((1,)),
            dma((count,)),
            dma((1,)),
            dma((count,)),
            dma((1,)),
        ],
        compiler_params=pltpu.CompilerParams(
            vmem_limit_bytes=60 * 1024 * 1024, collective_id=0, has_side_effects=True
        ),
    )(
        val_occupation, val_energy, cond_energy, gvectors,
        valence, conduction, left, right, sign, xtab,
    )
    all_pairs = slots * pairs
    prefactor = -1.0 / math.sqrt(all_pairs)
    return product(
        rows.reshape(all_pairs, span), cols.reshape(all_pairs, width), share, prefactor
    )


def either_body(valence, conduction, *rest):
    nv, planes, _ = valence.shape
    count = lax.axis_size("pair")
    width = 2 * KG // count
    fits = (
        count == lax.axis_size("grow")
        and count % 2 == 0
        and lax.axis_size("gcol") == 2
        and planes % 8 == 0
        and conduction.shape[0] == 2
        and 8 * nv == 128
        and width % PIECE == 0
        and width // PIECE % 2 == 1
        and KG // PIECE % UNIT == 0
    )
    return (fast_body if fits else body)(valence, conduction, *rest)


def solution(mesh):
    return jax.shard_map(
        either_body,
        mesh=mesh,
        in_specs=(P(None, "grow", None), P(("pair", "gcol"), "grow", None), P(), P(), P(), P()),
        out_specs=P(("pair", "gcol"), "grow"),
        check_vma=False,
    )
```
